128 devices in a mesh: row: 8 (over y, x_hi), col: 16 (over x_lo, z, core).
Axes of the slice: x: 4 (x_hi: 2, x_lo: 2; x = x_hi * 2 + x_lo), y: 4, z: 4, core: 2. Of those that a mesh axis runs over, the one named last changes fastest.
Arguments:
- initial_field: float32 [1, 1024, 8192], P(None, 'row', 'col'), may hold values from -12 to 12
- information: float32 [1024, 8192], P('row', 'col'), may hold values from -24 to 24
- kappa_squared: float32 [1024, 8192], P('row', 'col'), may hold values from 0.05 to 2
- lumped_mass: float32 [1024, 8192], P('row', 'col'), may hold values from 0.5 to 2
- noise_seeds: int32 [8, 16, 2, 4, 1], P('row', 'col'), may hold values from 0 to 1073741823
- colour_order: int32 [4], replicated, may hold values from 0 to 3, each once
Outputs:
- final_field: float32 [1, 1024, 8192], P(None, 'row', 'col')
- energies: float32 [2, 4, 1], replicated
The draws below stay inside these ranges and needn't reach their ends.
Inputs may be any that keep to these rules, and one draw needn't show every extreme that they name: `noise_seeds`: one seed for each tile of 128 x 512 nodes, sweep, colour phase and chain. `colour_order`: names each of the 4 block colours once.
All inputs are finite; a program needn't handle non-finite values.
Results may differ from the reference program's by a relative error of at most 0.0003.
Values sent between devices are 32-bit elements; how exact they have to be, the bound alone decides.
A program may use at most 128 MiB of HBM per device.

```python
import math
import jax
import jax.numpy as jnp
from jax import lax

TR = 128
TC = 512
CHAINS = 1
SWEEPS = 2
COLOURS = 4
NR = 1024
NC = 8192
ROW_TILES = 8
COL_TILES = 16


def ramp_scale():
    down_axis = jnp.arange(NR, dtype=jnp.float32) / NR
    across = jnp.arange(NC, dtype=jnp.float32) / NC
    return 1.0 + down_axis[:, None] + across[None, :]


def draw_initial_field(key, part):
    key = jax.random.fold_in(key, 17)
    values = jnp.clip(jax.random.normal(key, (CHAINS, NR, NC), jnp.float32), -4.0, 4.0)
    return values * ramp_scale()


def draw_information(key, part):
    key = jax.random.fold_in(key, 29)
    values = 2.0 * jnp.clip(jax.random.normal(key, (NR, NC), jnp.float32), -4.0, 4.0)
    return values * ramp_scale()


def plant(array, rng, least, largest):
    place = [jax.random.randint(jax.random.fold_in(rng, axis), (), 0, length) for axis, length in enumerate(array.shape)]
    longest = array.shape.index(max(array.shape))
    beside = place[:longest] + [(place[longest] + 1) % array.shape[longest]] + place[longest + 1:]
    return array.at[tuple(place)].set(least).at[tuple(beside)].set(largest)


def level_of(own_key, extent, split, smallest, largest):
    def one(axis_at, shards_of):
        steps = jax.random.uniform(jax.random.fold_in(jax.random.fold_in(own_key, 6), axis_at), (shards_of,), jnp.float32, smallest / len(split), largest / len(split))
        return jnp.repeat(jnp.exp(steps), extent[axis_at] // shards_of).reshape((-1,) + (1,) * (len(extent) - axis_at - 1))

    factor_of = one(*split[0])
    for cut in split[1:]:
        factor_of = factor_of * one(*cut)
    return factor_of


def setup_inputs(seed: int = 0) -> dict:
    keys = jax.random.split(jax.random.key(seed), 7)
    return {
        "initial_field": draw_initial_field(jax.random.fold_in(keys[6], 71), 0),
        "information": draw_information(jax.random.fold_in(keys[6], 71), 0),
        "kappa_squared": jnp.clip(jnp.exp(math.log(2.0) - 3.6888794 * jax.random.uniform(keys[2], (NR, NC), jnp.float32) ** level_of(keys[2], (NR, NC), ((0, 8), (1, 16)), -0.2, 0.2)), 0.05, 2.0),
        "lumped_mass": jnp.clip(jnp.exp(math.log(2.0) - 1.3862944 * jax.random.uniform(keys[3], (NR, NC), jnp.float32) ** level_of(keys[3], (NR, NC), ((0, 8), (1, 16)), -0.2, 0.2)), 0.5, 2.0),
        "noise_seeds": plant(jax.random.randint(keys[4], (ROW_TILES, COL_TILES, SWEEPS, COLOURS, CHAINS), 0, 1073741824), jax.random.fold_in(keys[4], 1), 0, 1073741823).astype(jnp.int32),
        "colour_order": jax.random.permutation(keys[5], COLOURS).astype(jnp.int32),
    }


full_turn = 6.283185307179586
unit_step = 1.0 / 8388608.0
mix_factor = 73244475

def neighbours(source):
    return jnp.roll(source, 1, axis=-2) + jnp.roll(source, -1, axis=-2) + jnp.roll(source, 1, axis=-1) + jnp.roll(source, -1, axis=-1)

def apply_precision(sample_field, stiffness, inverse):
    first_pass = stiffness * sample_field - neighbours(sample_field)
    scaled = inverse * first_pass
    return stiffness * scaled - neighbours(scaled)

def corners(source):
    leading = source.shape[:-2]
    height, breadth = (source.shape[-2], source.shape[-1])
    shaped = source.reshape(leading + (height // 2, 2, breadth // 2, 2))
    return [shaped[..., :, first_index, :, second_index] for first_index in (0, 1) for second_index in (0, 1)]

def join_corners(pieces):
    top_half = jnp.stack([pieces[0], pieces[1]], axis=-1)
    bottom_half = jnp.stack([pieces[2], pieces[3]], axis=-1)
    top_half = top_half.reshape(top_half.shape[:-2] + (top_half.shape[-2] * 2,))
    bottom_half = bottom_half.reshape(bottom_half.shape[:-2] + (bottom_half.shape[-2] * 2,))
    stacked = jnp.stack([top_half, bottom_half], axis=-2)
    return stacked.reshape(stacked.shape[:-3] + (stacked.shape[-3] * 2, stacked.shape[-1]))

def block_matrix(stiff_corners, inverse_corners, diagonal_corners):
    scaled = [stiff_corners[corner] * inverse_corners[corner] for corner in range(4)]
    matrix = [[None] * 4 for corner in range(4)]
    for corner in range(4):
        matrix[corner][corner] = diagonal_corners[corner]
    for first_index, second_index in ((0, 1), (0, 2), (1, 3), (2, 3)):
        element = -(scaled[first_index] + scaled[second_index])
        matrix[first_index][second_index] = element
        matrix[second_index][first_index] = element
    matrix[0][3] = inverse_corners[1] + inverse_corners[2]
    matrix[3][0] = matrix[0][3]
    matrix[1][2] = inverse_corners[0] + inverse_corners[3]
    matrix[2][1] = matrix[1][2]
    return matrix

def cholesky_rows(matrix):
    factor = [[None] * 4 for corner in range(4)]
    for first_index in range(4):
        for second_index in range(first_index + 1):
            running = matrix[first_index][second_index]
            for middle in range(second_index):
                running = running - factor[first_index][middle] * factor[second_index][middle]
            if first_index == second_index:
                factor[first_index][first_index] = jnp.sqrt(running)
            else:
                factor[first_index][second_index] = running / factor[second_index][second_index]
    return factor

def resample(field_corners, applied_corners, info_corners, matrix, factor, noise_list):
    right_side = []
    for first_index in range(4):
        coupled = matrix[first_index][0] * field_corners[0]
        for second_index in range(1, 4):
            coupled = coupled + matrix[first_index][second_index] * field_corners[second_index]
        right_side.append(info_corners[first_index] - applied_corners[first_index] + coupled)
    forward = []
    for first_index in range(4):
        running = right_side[first_index]
        for second_index in range(first_index):
            running = running - factor[first_index][second_index] * forward[second_index]
        forward.append(running / factor[first_index][first_index])
    shifted = [forward[corner] + noise_list[corner] for corner in range(4)]
    result = [None] * 4
    for first_index in reversed(range(4)):
        running = shifted[first_index]
        for second_index in range(first_index + 1, 4):
            running = running - factor[second_index][first_index] * result[second_index]
        result[first_index] = running / factor[first_index][first_index]
    return result

def scramble(hashed):
    sixteen = jnp.full_like(hashed, 16)
    hashed = hashed ^ lax.shift_right_logical(hashed, sixteen)
    hashed = hashed * mix_factor
    hashed = hashed ^ lax.shift_right_logical(hashed, sixteen)
    hashed = hashed * mix_factor
    return hashed ^ lax.shift_right_logical(hashed, sixteen)

def gaussian(seed_nodes, offsets):
    first_hash = scramble(seed_nodes + 2 * offsets)
    second_hash = scramble(seed_nodes + 2 * offsets + 1)
    shift_nine = jnp.full_like(first_hash, 9)
    uniform_one = (lax.shift_right_logical(first_hash, shift_nine).astype(jnp.float32) + 1.0) * unit_step
    uniform_two = lax.shift_right_logical(second_hash, shift_nine).astype(jnp.float32) * unit_step
    return jnp.sqrt(-2.0 * jnp.log(uniform_one)) * jnp.cos(full_turn * uniform_two)

def reference(initial_field, information, kappa_squared, lumped_mass, noise_seeds, colour_order):
    stiffness = kappa_squared * lumped_mass + 4.0
    inverse = 1.0 / lumped_mass
    diagonal = stiffness * stiffness * inverse + neighbours(inverse)
    matrix = block_matrix(corners(stiffness), corners(inverse), corners(diagonal))
    factor = cholesky_rows(matrix)
    info_corners = corners(information)
    half_rows = jnp.arange(NR // 2, dtype=jnp.int32)
    half_cols = jnp.arange(NC // 2, dtype=jnp.int32)
    block_colour = 2 * (half_rows % 2)[:, None] + (half_cols % 2)[None, :]
    offset_list = []
    tile_list = []
    for corner in range(4):
        node_rows = 2 * half_rows + corner // 2
        node_cols = 2 * half_cols + corner % 2
        offset_list.append((node_rows % TR)[:, None] * TC + (node_cols % TC)[None, :])
        tile_list.append((node_rows // TR, node_cols // TC))

    def one_sweep(sweep_index, loop_state):
        sample_field, energies = loop_state
        seed_layer = lax.dynamic_index_in_dim(noise_seeds, sweep_index, 2, keepdims=False)
        for phase_index in range(COLOURS):
            applied = apply_precision(sample_field, stiffness, inverse)
            energy = lax.optimization_barrier(jnp.sum(0.5 * sample_field * applied - information * sample_field, axis=(1, 2))) / (NR * NC)
            energies = energies.at[sweep_index, phase_index].set(energy)
            seed_table = seed_layer[:, :, phase_index, :]
            noise_list = []
            for corner in range(4):
                picked = seed_table[tile_list[corner][0]][:, tile_list[corner][1]]
                noise_list.append(gaussian(jnp.moveaxis(picked, -1, 0), offset_list[corner]))
            before = corners(sample_field)
            updated = resample(before, corners(applied), info_corners, matrix, factor, noise_list)
            chosen = block_colour == colour_order[phase_index]
            sample_field = join_corners([jnp.where(chosen, updated[corner], before[corner]) for corner in range(4)])
        return (sample_field, energies)
    initial = (initial_field, jnp.zeros((SWEEPS, COLOURS, CHAINS), jnp.float32))
    final_field, energies = lax.fori_loop(0, SWEEPS, one_sweep, initial)
    return (final_field, energies)
```

```python
import jax
import jax.numpy as jnp
from jax import lax
from jax.experimental import pallas as pl
from jax.experimental.pallas import tpu as pltpu
from jax.sharding import PartitionSpec as P

MESH = pl.DeviceIdType.MESH
SWEEPS = 2
COLOURS = 4
PHASES = SWEEPS * COLOURS
HALO = 16
TR = 128
TC = 512
EXT = TR + 2 * HALO
ROWS = EXT // 4
GROUPS = ROWS // 8
PAD = 8
PADDED = ROWS + 2 * PAD
LANES = 128
MIX = 73244475
STEP = 1.0 / 8388608.0
NODES = 8388608.0
NEIGHBOURS = [(a, b) for a in (-1, 0, 1) for b in (-1, 0, 1) if (a, b) != (0, 0)]
LOWER = {(1, 0): 4, (2, 0): 5, (2, 1): 6, (3, 0): 7, (3, 1): 8, (3, 2): 9}
SINE = (6.283185307179586, -41.34170224039976, 81.60524927607506, -76.70585975306136, 42.05869394489765, -15.09464257682298, 3.8199525848482803)


def tile():
    return lax.broadcasted_iota(jnp.int32, (8, LANES), 0), lax.broadcasted_iota(jnp.int32, (8, LANES), 1)


def logical(value, amount):
    return lax.shift_right_logical(value, jnp.full_like(value, amount))


def scramble(hashed):
    hashed = (hashed ^ logical(hashed, 16)) * MIX
    hashed = (hashed ^ logical(hashed, 16)) * MIX
    return hashed ^ logical(hashed, 16)


def gaussian(base):
    one = (logical(scramble(base), 9).astype(jnp.float32) + 1.0) * STEP
    two = logical(scramble(base + 1), 9).astype(jnp.float32) * STEP
    squared = -2.0 * jnp.log(one)
    radius = squared * lax.rsqrt(jnp.maximum(squared, 1e-30))
    turn = jnp.abs(two - 0.5) - 0.25
    square = turn * turn
    series = jnp.full_like(square, SINE[6])
    for n in range(5, -1, -1):
        series = series * square + SINE[n]
    return radius * (turn * series)


def lane_next(main, side, lane):
    main, side = pltpu.roll(main, LANES - 1, 1), pltpu.roll(side, LANES - 1, 1)
    last = lane == LANES - 1
    return jnp.where(last, side, main), jnp.where(last, main, side)


def lane_prev(main, side, lane):
    main, side = pltpu.roll(main, 1, 1), pltpu.roll(side, 1, 1)
    first = lane == 0
    return jnp.where(first, side, main), jnp.where(first, main, side)


def pick(index, lane_source):
    return jnp.take_along_axis(lane_source, index, axis=1, mode="promise_in_bounds")


def kernel(
    field_ref, info_ref, kappa_ref, mass_ref, seed_ref, order_ref, out_ref, energy_ref,
    nat, pack, strip_l, strip_r, seedbuf, seedmap, noise, fld, stf, inf, inv, scl, kd, fac, delta, acc, outn, e1, e2,
    load_sem, send_sem, recv_sem, store_sem, esend, erecv,
):
    r, c = lax.axis_index("row"), lax.axis_index("col")
    sub, lane = tile()

    def at(dr, dc):
        return (lax.rem(r + (dr + 8), 8), lax.rem(c + (dc + 16), 16))

    barrier = pltpu.get_barrier_semaphore()
    peers = [at(0, k) for k in range(1, 16)] + [at(k, 0) for k in range(1, 8)]
    peers += [at(a, b) for a in (-1, 1) for b in (-1, 1)]
    for peer in peers:
        pl.semaphore_signal(barrier, inc=1, device_id=peer, device_id_type=MESH)

    sources = (field_ref.at[0], info_ref, kappa_ref, mass_ref)
    loads = []
    for i in range(4):
        for k in range(4):
            loads.append(
                pltpu.make_async_copy(
                    sources[i].at[:, pl.ds(LANES * k, LANES)], nat.at[i, k, pl.ds(HALO, TR)], load_sem.at[i, k]
                )
            )
            loads[-1].start()

    own = jnp.zeros((8, LANES), jnp.int32)
    for t in range(SWEEPS):
        for colour in range(COLOURS):
            seed = jnp.int32(0)
            for k in range(COLOURS):
                seed = seed + jnp.where(order_ref[k] == colour, seed_ref[t * COLOURS + k], 0)
            own = jnp.where(sub == t * COLOURS + colour, seed, own)
    seedbuf[4] = own

    for load in loads:
        load.wait()

    def pack_rows(g, _):
        rows = pl.ds(HALO + 8 * g, 8)
        total = jnp.zeros((8, LANES), jnp.float32)
        for i in range(4):
            right = pltpu.roll(nat[i, 3, rows, :], 16 * i + 16, 1)
            left = pltpu.roll(nat[i, 0, rows, :], 64 + 16 * i, 1)
            total = jnp.where((lane >= 16 * i) & (lane < 16 * i + 16), right, total)
            total = jnp.where((lane >= 64 + 16 * i) & (lane < 80 + 16 * i), left, total)
        pack[pl.ds(8 * g, 8), :] = total
        return 0

    lax.fori_loop(0, TR // 8, pack_rows, 0)

    pl.semaphore_wait(barrier, len(peers))
    copies = []

    def send(source, target, where):
        n = len(copies)
        copies.append(
            pltpu.make_async_remote_copy(
                src_ref=source,
                dst_ref=target,
                send_sem=send_sem.at[n],
                recv_sem=recv_sem.at[n],
                device_id=at(*where),
                device_id_type=MESH,
            )
        )
        copies[-1].start()

    for dr, dc in NEIGHBOURS:
        send(seedbuf.at[4], seedbuf.at[(1 - dr) * 3 + 1 - dc], (dr, dc))
    for dr in (-1, 0, 1):
        mine = {-1: pl.ds(0, HALO), 0: pl.ds(0, TR), 1: pl.ds(TR - HALO, HALO)}[dr]
        theirs = {-1: pl.ds(HALO + TR, HALO), 0: pl.ds(HALO, TR), 1: pl.ds(0, HALO)}[dr]
        send(pack.at[mine], strip_l.at[theirs], (dr, 1))
        send(pack.at[mine], strip_r.at[theirs], (dr, -1))
    send(nat.at[:, :, pl.ds(HALO, HALO)], nat.at[:, :, pl.ds(HALO + TR, HALO)], (-1, 0))
    send(nat.at[:, :, pl.ds(TR, HALO)], nat.at[:, :, pl.ds(0, HALO)], (1, 0))

    zero = jnp.zeros((8, LANES), jnp.float32)

    def clear(n, _):
        for v in range(2):
            for buffer in (fld, inv, scl, kd):
                buffer[n, v, 0:PAD, :] = zero
                buffer[n, v, PAD + ROWS : PADDED, :] = zero
            for g in range(GROUPS):
                kd[n, v, PAD + 8 * g : PAD + 8 * g + 8, :] = zero
        return 0

    lax.fori_loop(0, 16, clear, 0)

    def draw(g, group_class, v):
        for rho in range(4):
            row = 4 * ((sub + (8 * g + 28)) & 31) + rho
            for kappa in range(4):
                colour = 2 * (rho // 2) + kappa // 2
                offset = 2 * (row * TC + 4 * lane + kappa)
                for t in range(SWEEPS):
                    seeds = seedmap[t * COLOURS + colour, v, group_class]
                    noise[t, 4 * rho + kappa, v, pl.ds(pl.multiple_of(8 * g, 8), 8), :] = gaussian(seeds + offset)

    def splat(slot, n):
        return jnp.broadcast_to(seedbuf[slot, n : n + 1, :], (8, LANES))

    for n in range(8):
        seedmap[n, 0, 1] = splat(4, n)

    def inner(g, _):
        draw(g, 1, 0)
        return 0

    lax.fori_loop(1, GROUPS - 1, inner, 0)

    for copy in copies[:8]:
        copy.wait()
    for n in range(8):
        seedmap[n, 0, 0] = jnp.where(sub < 4, splat(1, n), splat(4, n))
        seedmap[n, 0, 2] = jnp.where(sub < 4, splat(4, n), splat(7, n))
        rows = [jnp.where(lane < 64, splat(3 * a + 2, n), splat(3 * a, n)) for a in range(3)]
        seedmap[n, 1, 0] = jnp.where(sub < 4, rows[0], rows[1])
        seedmap[n, 1, 1] = rows[1]
        seedmap[n, 1, 2] = jnp.where(sub < 4, rows[1], rows[2])
    draw(0, 0, 0)
    draw(GROUPS - 1, 2, 0)

    def side(g, _):
        draw(g, jnp.where(g == 0, 0, jnp.where(g == GROUPS - 1, 2, 1)), 1)
        return 0

    lax.fori_loop(0, GROUPS, side, 0)

    for copy in copies[8:]:
        copy.wait()

    block = lane // 32
    split = [4 * (lane & 31) + ((block - k) & 3) for k in range(4)]
    edge = lane < 64
    used = (lane < 4) | (lane >= 124)

    def planes(g, _):
        rows = pl.ds(pl.multiple_of(8 * g, 8), 8)
        padded = pl.ds(pl.multiple_of(8 * g + PAD, 8), 8)
        for rho in range(4):
            natural = pl.ds(32 * g + rho, 8, stride=4)
            mixed = jnp.where(edge, strip_l[natural, :], strip_r[natural, :])
            values = []
            for i in range(4):
                chunks = [pick(split[k], nat[i, k, natural, :]) for k in range(4)]
                row = []
                for kappa in range(4):
                    m = chunks[(-kappa) & 3]
                    for b in range(1, 4):
                        m = jnp.where(block == b, chunks[(b - kappa) & 3], m)
                    main = pltpu.roll(m, (LANES - 32 * kappa) % LANES, 1) if kappa else m
                    index = jnp.where(edge, 64 + 16 * i + 4 * (lane & 3) + kappa, 16 * i + 4 * (lane & 3) + kappa)
                    filler = 0.0 if i < 2 else 1.0
                    row.append((main, jnp.where(used, pick(index, mixed), filler)))
                values.append(row)
            for kappa in range(4):
                n = 4 * rho + kappa
                for v in range(2):
                    mass = values[3][kappa][v]
                    fld[n, v, padded, :] = values[0][kappa][v]
                    inf[n, v, rows, :] = values[1][kappa][v]
                    stf[n, v, rows, :] = values[2][kappa][v] * mass + 4.0
                    inv[n, v, padded, :] = 1.0 / mass
        return 0

    lax.fori_loop(0, GROUPS, planes, 0)

    def around(ref, rho, kappa, base):
        up = (4 * ((rho + 3) % 4) + kappa, base - 1 if rho == 0 else base)
        down = (4 * ((rho + 1) % 4) + kappa, base + 1 if rho == 3 else base)
        here = pl.ds(base, 8)
        left = [ref[4 * rho + (kappa + 3) % 4, v, here, :] for v in range(2)]
        right = [ref[4 * rho + (kappa + 1) % 4, v, here, :] for v in range(2)]
        if kappa == 0:
            left = lane_prev(*left, lane)
        if kappa == 3:
            right = lane_next(*right, lane)
        return [
            ref[up[0], v, pl.ds(up[1], 8), :] + ref[down[0], v, pl.ds(down[1], 8), :] + left[v] + right[v]
            for v in range(2)
        ]

    def is_own(g):
        j = sub + 8 * g
        return (j >= 4) & (j < 36)

    def first(g, total):
        base = pl.multiple_of(8 * g + PAD, 8)
        rows = pl.ds(pl.multiple_of(8 * g, 8), 8)
        here = pl.ds(base, 8)
        part = zero
        for rho in range(4):
            for kappa in range(4):
                n = 4 * rho + kappa
                near = around(fld, rho, kappa, base)
                for v in range(2):
                    value = fld[n, v, here, :]
                    applied = stf[n, v, rows, :] * value - near[v]
                    scaled = inv[n, v, here, :] * applied
                    scl[n, v, here, :] = scaled
                    if v == 0:
                        part = part + (0.5 * scaled * applied - inf[n, v, rows, :] * value)
        return total + jnp.where(is_own(g), part, 0.0)

    acc[0] = lax.fori_loop(0, GROUPS, first, zero)

    def factors(g, _):
        base = pl.multiple_of(8 * g + PAD, 8)
        rows = pl.ds(pl.multiple_of(8 * g, 8), 8)
        here = pl.ds(base, 8)
        for colour in range(COLOURS):
            top, left = 2 * (colour // 2), 2 * (colour % 2)
            corner = [(top + n // 2, left + n % 2) for n in range(4)]
            near = [around(inv, rho, kappa, base) for rho, kappa in corner]
            for v in range(2):
                s = [stf[4 * rho + kappa, v, rows, :] for rho, kappa in corner]
                w = [inv[4 * rho + kappa, v, here, :] for rho, kappa in corner]
                sw = [s[n] * w[n] for n in range(4)]
                q = {(n, n): s[n] * sw[n] + near[n][v] for n in range(4)}
                for a, b in ((1, 0), (2, 0), (3, 1), (3, 2)):
                    q[a, b] = -(sw[a] + sw[b])
                q[3, 0] = w[1] + w[2]
                q[2, 1] = w[0] + w[3]
                low = {}
                for a in range(4):
                    for b in range(a + 1):
                        running = q[a, b]
                        for m in range(b):
                            running = running - low[a, m] * low[b, m]
                        low[a, b] = lax.rsqrt(running) if a == b else running * low[b, b]
                for n in range(4):
                    fac[n, colour, v, rows, :] = low[n, n]
                for (a, b), n in LOWER.items():
                    fac[n, colour, v, rows, :] = low[a, b]
        return 0

    lax.fori_loop(0, GROUPS, factors, 0)

    def resample(i, g, total, scatter):
        t, k = i // COLOURS, lax.rem(i, COLOURS)
        colour = order_ref[k]
        a, b = lax.shift_right_logical(colour, 1), colour & 1
        low_b = jnp.full((8, LANES), b, jnp.int32) == 0
        base = pl.multiple_of(8 * g + PAD, 8)
        rows = pl.ds(pl.multiple_of(8 * g, 8), 8)
        here = pl.ds(base, 8)
        rel_row = [2 * a, 2 * a + 1, (2 * a + 2) & 3, (2 * a + 3) & 3]
        rel_col = [2 * b, 2 * b + 1, (2 * b + 2) & 3, (2 * b + 3) & 3]
        above = pl.ds(base - jnp.where(a == 0, 1, 0), 8)
        below = pl.ds(base + jnp.where(a == 1, 1, 0), 8)

        def read(p, q, where=here):
            return [scl[4 * rel_row[p] + rel_col[q], v, where, :] for v in range(2)]

        node = [[read(p, q) for q in range(2)] for p in range(2)]
        up = [read(3, q, above) for q in range(2)]
        down = [read(2, q, below) for q in range(2)]
        left, right = [], []
        for p in range(2):
            raw = read(p, 3)
            moved = lane_prev(*raw, lane)
            left.append([jnp.where(low_b, moved[v], raw[v]) for v in range(2)])
            raw = read(p, 2)
            moved = lane_next(*raw, lane)
            right.append([jnp.where(low_b, raw[v], moved[v]) for v in range(2)])
        moves = []
        for v in range(2):
            f, drawn = [], []
            inverse = [fac[n, colour, v, rows, :] for n in range(4)]
            low = {key: fac[n, colour, v, rows, :] for key, n in LOWER.items()}
            for n in range(4):
                p, q = n // 2, n % 2
                place = 4 * rel_row[p] + rel_col[q]
                near = node[1 - p][q][v] + node[p][1 - q][v]
                near = near + (down if p else up)[q][v] + (right if q else left)[p][v]
                running = inf[place, v, rows, :] - stf[place, v, rows, :] * node[p][q][v] + near
                for m in range(n):
                    running = running - low[n, m] * f[m]
                f.append(running * inverse[n])
                drawn.append(noise[t, place, v, rows, :])
            target = [f[n] + drawn[n] for n in range(4)]
            if v == 0 and scatter:
                part = (drawn[0] - f[0]) * target[0]
                for n in range(1, 4):
                    part = part + (drawn[n] - f[n]) * target[n]
                total = total + jnp.where(is_own(g), 0.5 * part, 0.0)
            move = [None] * 4
            for n in reversed(range(4)):
                running = target[n]
                for m in range(n + 1, 4):
                    running = running - low[m, n] * move[m]
                move[n] = running * inverse[n]
                if v == 0:
                    delta[i, n, rows, :] = move[n]
            if scatter:
                for n in range(4):
                    p, q = n // 2, n % 2
                    place = 4 * rel_row[p] + rel_col[q]
                    kd[4 * p + q, v, here, :] = move[n ^ 1] + move[n ^ 2] - stf[place, v, rows, :] * move[n]
                for q in range(2):
                    kd[12 + q, v, here, :] = move[q]
                    kd[8 + q, v, here, :] = move[2 + q]
            moves.append(move)
        if scatter:
            for p in range(2):
                raw = [moves[v][2 * p] for v in range(2)]
                moved = lane_next(*raw, lane)
                for v in range(2):
                    kd[4 * p + 3, v, here, :] = jnp.where(low_b, moved[v], raw[v])
                raw = [moves[v][2 * p + 1] for v in range(2)]
                moved = lane_prev(*raw, lane)
                for v in range(2):
                    kd[4 * p + 2, v, here, :] = jnp.where(low_b, raw[v], moved[v])
        return total

    def spread(i, g):
        colour = order_ref[lax.rem(i, COLOURS)]
        a, b = lax.shift_right_logical(colour, 1), colour & 1
        base = pl.multiple_of(8 * g + PAD, 8)
        here = pl.ds(base, 8)
        for rho in range(4):
            where = here
            if rho == 3:
                where = pl.ds(base + jnp.where(a == 0, 1, 0), 8)
            if rho == 0:
                where = pl.ds(base - jnp.where(a == 1, 1, 0), 8)
            for kappa in range(4):
                n = 4 * rho + kappa
                place = 4 * ((rho + 4 - 2 * a) & 3) + ((kappa + 4 - 2 * b) & 3)
                for v in range(2):
                    scl[n, v, here, :] = scl[n, v, here, :] - inv[n, v, here, :] * kd[place, v, where, :]

    def phase(i, _):
        acc[i + 1] = lax.fori_loop(0, GROUPS, lambda g, total: resample(i, g, total, True), zero)
        lax.fori_loop(0, GROUPS, lambda g, _: (spread(i, g), 0)[1], 0)
        return 0

    lax.fori_loop(0, PHASES - 1, phase, 0)

    line = jnp.zeros((1, LANES), jnp.float32)
    for k in range(PHASES):
        change = jnp.sum(jnp.sum(acc[k], axis=0, keepdims=True), axis=1, keepdims=True)
        line = line + jnp.where(lane[0:1] >= k, change, 0.0)
    e1[pl.ds(c, 1), :] = line
    for k in range(1, 16):
        pltpu.make_async_remote_copy(
            src_ref=e1.at[pl.ds(c, 1)], dst_ref=e1.at[pl.ds(c, 1)], send_sem=esend.at[0], recv_sem=erecv.at[0],
            device_id=at(0, k), device_id_type=MESH,
        ).start()

    lax.fori_loop(0, GROUPS, lambda g, total: resample(PHASES - 1, g, total, False), zero)

    turn_of = []
    for colour in range(COLOURS):
        turn = jnp.int32(0)
        for k in range(COLOURS):
            turn = jnp.where(order_ref[k] == colour, jnp.int32(k), turn)
        turn_of.append(turn)
    merge = [32 * (((lane & 3) + k) & 3) + lane // 4 for k in range(4)]

    def natural_rows(h, _):
        for rho in range(4):
            shifted = []
            for kappa in range(4):
                turn = turn_of[2 * (rho // 2) + kappa // 2]
                n = 2 * (rho % 2) + kappa % 2
                value = fld[4 * rho + kappa, 0, pl.ds(8 * h + PAD + 4, 8), :]
                value = value + delta[turn, n, pl.ds(8 * h + 4, 8), :]
                value = value + delta[turn + COLOURS, n, pl.ds(8 * h + 4, 8), :]
                shifted.append(pltpu.roll(value, 32 * kappa, 1) if kappa else value)
            for k in range(4):
                m = shifted[(-k) & 3]
                for b in range(1, 4):
                    m = jnp.where(block == b, shifted[(b - k) & 3], m)
                outn[k, pl.ds(32 * h + rho, 8, stride=4), :] = pick(merge[k], m)
        return 0

    lax.fori_loop(0, 4, natural_rows, 0)
    stores = [
        pltpu.make_async_copy(outn.at[k], out_ref.at[0, :, pl.ds(LANES * k, LANES)], store_sem.at[k]) for k in range(4)
    ]
    for store in stores:
        store.start()

    def finish(buffer, count, sem, where):
        pltpu.make_async_remote_copy(
            src_ref=buffer.at[pl.ds(0, count)], dst_ref=buffer.at[pl.ds(0, count)], send_sem=esend.at[sem],
            recv_sem=erecv.at[sem], device_id=where, device_id_type=MESH,
        ).wait()

    finish(e1, 15, 0, at(0, 1))
    e2[pl.ds(r, 1), :] = jnp.sum(e1[...], axis=0, keepdims=True)
    for k in range(1, 8):
        pltpu.make_async_remote_copy(
            src_ref=e2.at[pl.ds(r, 1)], dst_ref=e2.at[pl.ds(r, 1)], send_sem=esend.at[1], recv_sem=erecv.at[1],
            device_id=at(k, 0), device_id_type=MESH,
        ).start()
    finish(e2, 7, 1, at(1, 0))
    energy_ref[...] = jnp.broadcast_to(jnp.sum(e2[...], axis=0, keepdims=True) * (1.0 / NODES), (8, LANES))
    for store in stores:
        store.wait()


def local(initial_field, information, kappa_squared, lumped_mass, noise_seeds, colour_order):
    f32, i32 = jnp.float32, jnp.int32
    anywhere = pl.BlockSpec(memory_space=pl.ANY)
    scalar = pl.BlockSpec(memory_space=pltpu.SMEM)
    dma = pltpu.SemaphoreType.DMA
    final_field, energies = pl.pallas_call(
        kernel,
        out_shape=(jax.ShapeDtypeStruct((1, TR, TC), f32), jax.ShapeDtypeStruct((8, LANES), f32)),
        in_specs=[anywhere] * 4 + [scalar] * 2,
        out_specs=(anywhere, pl.BlockSpec(memory_space=pltpu.VMEM)),
        scratch_shapes=[
            pltpu.VMEM((4, 4, EXT, LANES), f32),
            pltpu.VMEM((TR, LANES), f32),
            pltpu.VMEM((EXT, LANES), f32),
            pltpu.VMEM((EXT, LANES), f32),
            pltpu.VMEM((9, 8, LANES), i32),
            pltpu.VMEM((8, 2, 3, 8, LANES), i32),
            pltpu.VMEM((SWEEPS, 16, 2, ROWS, LANES), f32),
            pltpu.VMEM((16, 2, PADDED, LANES), f32),
            pltpu.VMEM((16, 2, ROWS, LANES), f32),
            pltpu.VMEM((16, 2, ROWS, LANES), f32),
            pltpu.VMEM((16, 2, PADDED, LANES), f32),
            pltpu.VMEM((16, 2, PADDED, LANES), f32),
            pltpu.VMEM((16, 2, PADDED, LANES), f32),
            pltpu.VMEM((10, COLOURS, 2, ROWS, LANES), f32),
            pltpu.VMEM((PHASES, 4, ROWS, LANES), f32),
            pltpu.VMEM((PHASES, 8, LANES), f32),
            pltpu.VMEM((4, TR, LANES), f32),
            pltpu.VMEM((16, LANES), f32),
            pltpu.VMEM((8, LANES), f32),
            dma((4, 4)),
            dma((16,)),
            dma((16,)),
            dma((4,)),
            dma((2,)),
            dma((2,)),
        ],
        compiler_params=pltpu.CompilerParams(collective_id=0, has_side_effects=True),
        name="gibbs",
    )(initial_field, information, kappa_squared, lumped_mass, noise_seeds.reshape(PHASES), colour_order)
    return final_field, energies[0, :PHASES].reshape(SWEEPS, COLOURS, 1)


def solution(mesh):
    placed = (
        P(None, "row", "col"),
        P("row", "col"),
        P("row", "col"),
        P("row", "col"),
        P("row", "col", None, None, None),
        P(),
    )
    return jax.shard_map(
        local, mesh=mesh, in_specs=placed, out_specs=(P(None, "row", "col"), P()), check_vma=False
    )
```

```python
import jax
import jax.numpy as jnp
from jax import lax
from jax.experimental import pallas as pl
from jax.experimental.pallas import tpu as pltpu
from jax.sharding import PartitionSpec as P

MESH = pl.DeviceIdType.MESH
SWEEPS = 2
COLOURS = 4
PHASES = SWEEPS * COLOURS
HALO = 16
TR = 128
TC = 512
EXT = TR + 2 * HALO
ROWS = EXT // 4
GROUPS = ROWS // 8
PAD = 8
PADDED = ROWS + 2 * PAD
LANES = 128
MIX = 73244475
VMEM_LIMIT = 16 * 1024 * 1024
STEP = 1.0 / 8388608.0
NODES = 8388608.0
NEIGHBOURS = [(a, b) for a in (-1, 0, 1) for b in (-1, 0, 1) if (a, b) != (0, 0)]
LOWER = {(1, 0): 4, (2, 0): 5, (2, 1): 6, (3, 0): 7, (3, 1): 8, (3, 2): 9}
SINE = (6.283185307179586, -41.34170224039976, 81.60524927607506, -76.70585975306136, 42.05869394489765, -15.09464257682298, 3.8199525848482803)


def tile():
    return lax.broadcasted_iota(jnp.int32, (8, LANES), 0), lax.broadcasted_iota(jnp.int32, (8, LANES), 1)


def logical(value, amount):
    return lax.shift_right_logical(value, jnp.full_like(value, amount))


def scramble(hashed):
    hashed = (hashed ^ logical(hashed, 16)) * MIX
    hashed = (hashed ^ logical(hashed, 16)) * MIX
    return hashed ^ logical(hashed, 16)


def gaussian(base):
    one = (logical(scramble(base), 9).astype(jnp.float32) + 1.0) * STEP
    two = logical(scramble(base + 1), 9).astype(jnp.float32) * STEP
    squared = -2.0 * jnp.log(one)
    radius = squared * lax.rsqrt(jnp.maximum(squared, 1e-30))
    turn = jnp.abs(two - 0.5) - 0.25
    square = turn * turn
    series = jnp.full_like(square, SINE[6])
    for n in range(5, -1, -1):
        series = series * square + SINE[n]
    return radius * (turn * series)


def lane_next(main, side, lane):
    main, side = pltpu.roll(main, LANES - 1, 1), pltpu.roll(side, LANES - 1, 1)
    last = lane == LANES - 1
    return jnp.where(last, side, main), jnp.where(last, main, side)


def lane_prev(main, side, lane):
    main, side = pltpu.roll(main, 1, 1), pltpu.roll(side, 1, 1)
    first = lane == 0
    return jnp.where(first, side, main), jnp.where(first, main, side)


def pick(index, lane_source):
    return jnp.take_along_axis(lane_source, index, axis=1, mode="promise_in_bounds")


def kernel(
    field_ref, info_ref, kappa_ref, mass_ref, seed_ref, order_ref, outn, energy_ref,
    nat, pack, strip_l, strip_r, seedbuf, seedmap, noise, fld, stf, inf, inv, scl, kd, fac, delta, acc, e1, e2,
    load_sem, send_sem, recv_sem, esend, erecv,
):
    r, c = lax.axis_index("row"), lax.axis_index("col")
    sub, lane = tile()

    def at(dr, dc):
        return (lax.rem(r + (dr + 8), 8), lax.rem(c + (dc + 16), 16))

    barrier = pltpu.get_barrier_semaphore()
    peers = [at(*where) for where in NEIGHBOURS]
    peers += [at(0, k) for k in range(2, 15)] + [at(k, 0) for k in range(2, 7)]
    for peer in peers:
        pl.semaphore_signal(barrier, inc=1, device_id=peer, device_id_type=MESH)

    sources = (field_ref.at[0], info_ref, kappa_ref, mass_ref)
    loads = []
    for i in range(4):
        for k in range(4):
            loads.append(
                pltpu.make_async_copy(
                    sources[i].at[:, pl.ds(LANES * k, LANES)], nat.at[i, k, pl.ds(HALO, TR)], load_sem.at[i, k]
                )
            )
            loads[-1].start()

    own = jnp.zeros((8, LANES), jnp.int32)
    for t in range(SWEEPS):
        for colour in range(COLOURS):
            seed = jnp.int32(0)
            for k in range(COLOURS):
                seed = seed + jnp.where(order_ref[k] == colour, seed_ref[t, 0, k], 0)
            own = jnp.where(sub == t * COLOURS + colour, seed, own)
    seedbuf[4] = own

    for load in loads:
        load.wait()

    def pack_rows(g, _):
        rows = pl.ds(HALO + 8 * g, 8)
        total = jnp.zeros((8, LANES), jnp.float32)
        for i in range(4):
            right = pltpu.roll(nat[i, 3, rows, :], 16 * i + 16, 1)
            left = pltpu.roll(nat[i, 0, rows, :], 64 + 16 * i, 1)
            total = jnp.where((lane >= 16 * i) & (lane < 16 * i + 16), right, total)
            total = jnp.where((lane >= 64 + 16 * i) & (lane < 80 + 16 * i), left, total)
        pack[pl.ds(8 * g, 8), :] = total
        return 0

    lax.fori_loop(0, TR // 8, pack_rows, 0)

    pl.semaphore_wait(barrier, len(peers))
    copies = []

    def send(source, target, where):
        n = len(copies)
        copies.append(
            pltpu.make_async_remote_copy(
                src_ref=source,
                dst_ref=target,
                send_sem=send_sem.at[n],
                recv_sem=recv_sem.at[n],
                device_id=at(*where),
                device_id_type=MESH,
            )
        )
        copies[-1].start()

    for dr, dc in NEIGHBOURS:
        send(seedbuf.at[4], seedbuf.at[(1 - dr) * 3 + 1 - dc], (dr, dc))
    for dr in (-1, 0, 1):
        mine = {-1: pl.ds(0, HALO), 0: pl.ds(0, TR), 1: pl.ds(TR - HALO, HALO)}[dr]
        theirs = {-1: pl.ds(HALO + TR, HALO), 0: pl.ds(HALO, TR), 1: pl.ds(0, HALO)}[dr]
        send(pack.at[mine], strip_l.at[theirs], (dr, 1))
        send(pack.at[mine], strip_r.at[theirs], (dr, -1))
    send(nat.at[:, :, pl.ds(HALO, HALO)], nat.at[:, :, pl.ds(HALO + TR, HALO)], (-1, 0))
    send(nat.at[:, :, pl.ds(TR, HALO)], nat.at[:, :, pl.ds(0, HALO)], (1, 0))

    zero = jnp.zeros((8, LANES), jnp.float32)

    def clear(n, _):
        for v in range(2):
            for buffer in (fld, inv, scl, kd):
                buffer[n, v, 0:PAD, :] = zero
                buffer[n, v, PAD + ROWS : PADDED, :] = zero
            for g in range(GROUPS):
                kd[n, v, PAD + 8 * g : PAD + 8 * g + 8, :] = zero
        return 0

    lax.fori_loop(0, 16, clear, 0)

    block = lane // 32
    split = [4 * (lane & 31) + ((block - k) & 3) for k in range(4)]
    edge = lane < 64
    used = (lane < 4) | (lane >= 124)

    def keep(n, v, g, values):
        rows = pl.ds(8 * g, 8)
        padded = pl.ds(8 * g + PAD, 8)
        fld[n, v, padded, :] = values[0]
        inf[n, v, rows, :] = values[1]
        stf[n, v, rows, :] = values[2] * values[3] + 4.0
        inv[n, v, padded, :] = 1.0 / values[3]

    def main_planes(g):
        for rho in range(4):
            natural = pl.ds(32 * g + rho, 8, stride=4)
            values = []
            for i in range(4):
                chunks = [pick(split[k], nat[i, k, natural, :]) for k in range(4)]
                row = []
                for kappa in range(4):
                    m = chunks[(-kappa) & 3]
                    for b in range(1, 4):
                        m = jnp.where(block == b, chunks[(b - kappa) & 3], m)
                    row.append(pltpu.roll(m, LANES - 32 * kappa, 1) if kappa else m)
                values.append(row)
            for kappa in range(4):
                keep(4 * rho + kappa, 0, g, [values[i][kappa] for i in range(4)])

    def side_planes(g):
        for rho in range(4):
            natural = pl.ds(32 * g + rho, 8, stride=4)
            mixed = jnp.where(edge, strip_l[natural, :], strip_r[natural, :])
            for kappa in range(4):
                values = []
                for i in range(4):
                    index = 16 * i + 4 * (lane & 3) + kappa + jnp.where(edge, 64, 0)
                    values.append(jnp.where(used, pick(index, mixed), 0.0 if i < 2 else 1.0))
                keep(4 * rho + kappa, 1, g, values)

    def draw(g, group_class, v):
        for rho in range(4):
            row = 4 * ((sub + (8 * g + 28)) & 31) + rho
            for kappa in range(4):
                colour = 2 * (rho // 2) + kappa // 2
                offset = 2 * (row * TC + 4 * lane + kappa)
                for t in range(SWEEPS):
                    seeds = seedmap[t * COLOURS + colour, v, group_class]
                    noise[t, 4 * rho + kappa, v, pl.ds(pl.multiple_of(8 * g, 8), 8), :] = gaussian(seeds + offset)

    def splat(slot, n):
        return jnp.broadcast_to(seedbuf[slot, n : n + 1, :], (8, LANES))

    for n in range(8):
        seedmap[n, 0, 1] = splat(4, n)

    def inner(g, _):
        draw(g, 1, 0)
        return 0

    lax.fori_loop(1, GROUPS - 1, inner, 0)

    for copy in copies[:8]:
        copy.wait()
    for n in range(8):
        seedmap[n, 0, 0] = jnp.where(sub < 4, splat(1, n), splat(4, n))
        seedmap[n, 0, 2] = jnp.where(sub < 4, splat(4, n), splat(7, n))
        rows = [jnp.where(lane < 64, splat(3 * a + 2, n), splat(3 * a, n)) for a in range(3)]
        seedmap[n, 1, 0] = jnp.where(sub < 4, rows[0], rows[1])
        seedmap[n, 1, 1] = rows[1]
        seedmap[n, 1, 2] = jnp.where(sub < 4, rows[1], rows[2])
    draw(0, 0, 0)
    draw(GROUPS - 1, 2, 0)

    def side(g, _):
        draw(g, jnp.where(g == 0, 0, jnp.where(g == GROUPS - 1, 2, 1)), 1)
        return 0

    lax.fori_loop(0, GROUPS, side, 0)

    for g in range(1, GROUPS - 1):
        main_planes(g)
    for copy in copies[8:14]:
        copy.wait()
    for g in range(GROUPS):
        side_planes(g)
    for copy in copies[14:]:
        copy.wait()
    for g in (0, GROUPS - 1):
        main_planes(g)

    def around(ref, rho, kappa, base):
        up = (4 * ((rho + 3) % 4) + kappa, base - 1 if rho == 0 else base)
        down = (4 * ((rho + 1) % 4) + kappa, base + 1 if rho == 3 else base)
        here = pl.ds(base, 8)
        left = [ref[4 * rho + (kappa + 3) % 4, v, here, :] for v in range(2)]
        right = [ref[4 * rho + (kappa + 1) % 4, v, here, :] for v in range(2)]
        if kappa == 0:
            left = lane_prev(*left, lane)
        if kappa == 3:
            right = lane_next(*right, lane)
        return [
            ref[up[0], v, pl.ds(up[1], 8), :] + ref[down[0], v, pl.ds(down[1], 8), :] + left[v] + right[v]
            for v in range(2)
        ]

    def sweep(step):
        total = zero
        for g in range(GROUPS):
            total = step(g, total)
        return total

    def is_own(g):
        j = sub + 8 * g
        return (j >= 4) & (j < 36)

    def first(g, total):
        base = 8 * g + PAD
        rows = pl.ds(8 * g, 8)
        here = pl.ds(base, 8)
        part = zero
        for rho in range(4):
            for kappa in range(4):
                n = 4 * rho + kappa
                near = around(fld, rho, kappa, base)
                for v in range(2):
                    value = fld[n, v, here, :]
                    applied = stf[n, v, rows, :] * value - near[v]
                    scaled = inv[n, v, here, :] * applied
                    scl[n, v, here, :] = scaled
                    if v == 0:
                        part = part + (0.5 * scaled * applied - inf[n, v, rows, :] * value)
        return total + jnp.where(is_own(g), part, 0.0)

    acc[0] = sweep(first)

    def factors(g):
        base = 8 * g + PAD
        rows = pl.ds(8 * g, 8)
        here = pl.ds(base, 8)
        for colour in range(COLOURS):
            top, left = 2 * (colour // 2), 2 * (colour % 2)
            corner = [(top + n // 2, left + n % 2) for n in range(4)]
            near = [around(inv, rho, kappa, base) for rho, kappa in corner]
            for v in range(2):
                s = [stf[4 * rho + kappa, v, rows, :] for rho, kappa in corner]
                w = [inv[4 * rho + kappa, v, here, :] for rho, kappa in corner]
                sw = [s[n] * w[n] for n in range(4)]
                q = {(n, n): s[n] * sw[n] + near[n][v] for n in range(4)}
                for a, b in ((1, 0), (2, 0), (3, 1), (3, 2)):
                    q[a, b] = -(sw[a] + sw[b])
                q[3, 0] = w[1] + w[2]
                q[2, 1] = w[0] + w[3]
                low = {}
                for a in range(4):
                    for b in range(a + 1):
                        running = q[a, b]
                        for m in range(b):
                            running = running - low[a, m] * low[b, m]
                        low[a, b] = lax.rsqrt(running) if a == b else running * low[b, b]
                for n in range(4):
                    fac[n, colour, v, rows, :] = low[n, n]
                for (a, b), n in LOWER.items():
                    fac[n, colour, v, rows, :] = low[a, b]

    for g in range(GROUPS):
        factors(g)

    def resample(i, g, total, scatter):
        t, k = i // COLOURS, lax.rem(i, COLOURS)
        colour = order_ref[k]
        a, b = lax.shift_right_logical(colour, 1), colour & 1
        low_b = jnp.full((8, LANES), b, jnp.int32) == 0
        base = 8 * g + PAD
        rows = pl.ds(8 * g, 8)
        here = pl.ds(base, 8)
        rel_row = [2 * a, 2 * a + 1, (2 * a + 2) & 3, (2 * a + 3) & 3]
        rel_col = [2 * b, 2 * b + 1, (2 * b + 2) & 3, (2 * b + 3) & 3]
        above = pl.ds(base - jnp.where(a == 0, 1, 0), 8)
        below = pl.ds(base + jnp.where(a == 1, 1, 0), 8)

        def read(p, q, where=here):
            return [scl[4 * rel_row[p] + rel_col[q], v, where, :] for v in range(2)]

        node = [[read(p, q) for q in range(2)] for p in range(2)]
        up = [read(3, q, above) for q in range(2)]
        down = [read(2, q, below) for q in range(2)]
        left, right = [], []
        for p in range(2):
            raw = read(p, 3)
            moved = lane_prev(*raw, lane)
            left.append([jnp.where(low_b, moved[v], raw[v]) for v in range(2)])
            raw = read(p, 2)
            moved = lane_next(*raw, lane)
            right.append([jnp.where(low_b, raw[v], moved[v]) for v in range(2)])
        moves = []
        for v in range(2):
            f, drawn = [], []
            inverse = [fac[n, colour, v, rows, :] for n in range(4)]
            low = {key: fac[n, colour, v, rows, :] for key, n in LOWER.items()}
            for n in range(4):
                p, q = n // 2, n % 2
                place = 4 * rel_row[p] + rel_col[q]
                near = node[1 - p][q][v] + node[p][1 - q][v]
                near = near + (down if p else up)[q][v] + (right if q else left)[p][v]
                running = inf[place, v, rows, :] - stf[place, v, rows, :] * node[p][q][v] + near
                for m in range(n):
                    running = running - low[n, m] * f[m]
                f.append(running * inverse[n])
                drawn.append(noise[t, place, v, rows, :])
            target = [f[n] + drawn[n] for n in range(4)]
            if v == 0 and scatter:
                part = (drawn[0] - f[0]) * target[0]
                for n in range(1, 4):
                    part = part + (drawn[n] - f[n]) * target[n]
                total = total + jnp.where(is_own(g), 0.5 * part, 0.0)
            move = [None] * 4
            for n in reversed(range(4)):
                running = target[n]
                for m in range(n + 1, 4):
                    running = running - low[m, n] * move[m]
                move[n] = running * inverse[n]
                if v == 0:
                    delta[i, n, rows, :] = move[n]
            if scatter:
                for n in range(4):
                    p, q = n // 2, n % 2
                    place = 4 * rel_row[p] + rel_col[q]
                    kd[4 * p + q, v, here, :] = move[n ^ 1] + move[n ^ 2] - stf[place, v, rows, :] * move[n]
                for q in range(2):
                    kd[12 + q, v, here, :] = move[q]
                    kd[8 + q, v, here, :] = move[2 + q]
            moves.append(move)
        if scatter:
            for p in range(2):
                raw = [moves[v][2 * p] for v in range(2)]
                moved = lane_next(*raw, lane)
                for v in range(2):
                    kd[4 * p + 3, v, here, :] = jnp.where(low_b, moved[v], raw[v])
                raw = [moves[v][2 * p + 1] for v in range(2)]
                moved = lane_prev(*raw, lane)
                for v in range(2):
                    kd[4 * p + 2, v, here, :] = jnp.where(low_b, raw[v], moved[v])
        return total

    def spread(i, g):
        colour = order_ref[lax.rem(i, COLOURS)]
        a, b = lax.shift_right_logical(colour, 1), colour & 1
        base = 8 * g + PAD
        here = pl.ds(base, 8)
        for rho in range(4):
            where = here
            if rho == 3:
                where = pl.ds(base + jnp.where(a == 0, 1, 0), 8)
            if rho == 0:
                where = pl.ds(base - jnp.where(a == 1, 1, 0), 8)
            for kappa in range(4):
                n = 4 * rho + kappa
                place = 4 * ((rho + 4 - 2 * a) & 3) + ((kappa + 4 - 2 * b) & 3)
                for v in range(2):
                    scl[n, v, here, :] = scl[n, v, here, :] - inv[n, v, here, :] * kd[place, v, where, :]

    def phase(i, _):
        acc[i + 1] = sweep(lambda g, total: resample(i, g, total, True))
        for g in range(GROUPS):
            spread(i, g)
        return 0

    lax.fori_loop(0, PHASES - 1, phase, 0)

    line = jnp.zeros((1, LANES), jnp.float32)
    for k in range(PHASES):
        change = jnp.sum(jnp.sum(acc[k], axis=0, keepdims=True), axis=1, keepdims=True)
        line = line + jnp.where(lane[0:1] >= k, change, 0.0)
    e1[pl.ds(c, 1), :] = line
    for k in range(1, 16):
        pltpu.make_async_remote_copy(
            src_ref=e1.at[pl.ds(c, 1)], dst_ref=e1.at[pl.ds(c, 1)], send_sem=esend.at[0], recv_sem=erecv.at[0],
            device_id=at(0, k), device_id_type=MESH,
        ).start()

    sweep(lambda g, total: resample(PHASES - 1, g, total, False))

    turn_of = []
    for colour in range(COLOURS):
        turn = jnp.int32(0)
        for k in range(COLOURS):
            turn = jnp.where(order_ref[k] == colour, jnp.int32(k), turn)
        turn_of.append(turn)
    merge = [32 * (((lane & 3) + k) & 3) + lane // 4 for k in range(4)]

    def natural_rows(h, _):
        for rho in range(4):
            shifted = []
            for kappa in range(4):
                turn = turn_of[2 * (rho // 2) + kappa // 2]
                n = 2 * (rho % 2) + kappa % 2
                value = fld[4 * rho + kappa, 0, pl.ds(8 * h + PAD + 4, 8), :]
                value = value + delta[turn, n, pl.ds(8 * h + 4, 8), :]
                value = value + delta[turn + COLOURS, n, pl.ds(8 * h + 4, 8), :]
                shifted.append(pltpu.roll(value, 32 * kappa, 1) if kappa else value)
            for k in range(4):
                m = shifted[(-k) & 3]
                for b in range(1, 4):
                    m = jnp.where(block == b, shifted[(b - k) & 3], m)
                outn[k, pl.ds(32 * h + rho, 8, stride=4), :] = pick(merge[k], m)
        return 0

    lax.fori_loop(0, 4, natural_rows, 0)
    def finish(buffer, count, sem, where):
        pltpu.make_async_remote_copy(
            src_ref=buffer.at[pl.ds(0, count)], dst_ref=buffer.at[pl.ds(0, count)], send_sem=esend.at[sem],
            recv_sem=erecv.at[sem], device_id=where, device_id_type=MESH,
        ).wait()

    finish(e1, 15, 0, at(0, 1))
    e2[pl.ds(r, 1), :] = jnp.sum(e1[...], axis=0, keepdims=True)
    for k in range(1, 8):
        pltpu.make_async_remote_copy(
            src_ref=e2.at[pl.ds(r, 1)], dst_ref=e2.at[pl.ds(r, 1)], send_sem=esend.at[1], recv_sem=erecv.at[1],
            device_id=at(k, 0), device_id_type=MESH,
        ).start()
    finish(e2, 7, 1, at(1, 0))
    energy_ref[...] = jnp.broadcast_to(jnp.sum(e2[...], axis=0, keepdims=True) * (1.0 / NODES), (8, LANES))


def deliver(field_ref, energy_ref, out_ref, out_energy_ref, store_sem):
    stores = [
        pltpu.make_async_copy(field_ref.at[k], out_ref.at[0, :, pl.ds(LANES * k, LANES)], store_sem.at[k])
        for k in range(4)
    ]
    for store in stores:
        store.start()
    line = energy_ref[0:1, :]
    out_energy_ref[0] = line[:, 0:COLOURS]
    out_energy_ref[1] = pltpu.roll(line, LANES - COLOURS, 1)[:, 0:COLOURS]
    for store in stores:
        store.wait()


def local(initial_field, information, kappa_squared, lumped_mass, noise_seeds, colour_order):
    f32, i32 = jnp.float32, jnp.int32
    anywhere = pl.BlockSpec(memory_space=pltpu.HBM)
    scalar = pl.BlockSpec(memory_space=pltpu.SMEM)
    dma = pltpu.SemaphoreType.DMA
    seeds = noise_seeds.reshape(SWEEPS, COLOURS, 1).transpose(0, 2, 1)
    vmem = pl.BlockSpec(memory_space=pltpu.VMEM)
    arrays = (initial_field, information, kappa_squared, lumped_mass)
    chunks, line = pl.pallas_call(
        kernel,
        out_shape=(jax.ShapeDtypeStruct((4, TR, LANES), f32), jax.ShapeDtypeStruct((8, LANES), f32)),
        in_specs=[anywhere] * 4 + [scalar] * 2,
        out_specs=(vmem, vmem),
        scratch_shapes=[
            pltpu.VMEM((4, 4, EXT, LANES), f32),
            pltpu.VMEM((TR, LANES), f32),
            pltpu.VMEM((EXT, LANES), f32),
            pltpu.VMEM((EXT, LANES), f32),
            pltpu.VMEM((9, 8, LANES), i32),
            pltpu.VMEM((8, 2, 3, 8, LANES), i32),
            pltpu.VMEM((SWEEPS, 16, 2, ROWS, LANES), f32),
            pltpu.VMEM((16, 2, PADDED, LANES), f32),
            pltpu.VMEM((16, 2, ROWS, LANES), f32),
            pltpu.VMEM((16, 2, ROWS, LANES), f32),
            pltpu.VMEM((16, 2, PADDED, LANES), f32),
            pltpu.VMEM((16, 2, PADDED, LANES), f32),
            pltpu.VMEM((16, 2, PADDED, LANES), f32),
            pltpu.VMEM((10, COLOURS, 2, ROWS, LANES), f32),
            pltpu.VMEM((PHASES, 4, ROWS, LANES), f32),
            pltpu.VMEM((PHASES, 8, LANES), f32),
            pltpu.VMEM((16, LANES), f32),
            pltpu.VMEM((8, LANES), f32),
            dma((4, 4)),
            dma((16,)),
            dma((16,)),
            dma((2,)),
            dma((2,)),
        ],
        compiler_params=pltpu.CompilerParams(collective_id=0, has_side_effects=True, vmem_limit_bytes=VMEM_LIMIT),
        name="gibbs",
    )(*(pltpu.with_memory_space_constraint(a, pltpu.HBM) for a in (*arrays, seeds, colour_order)))
    final_field, energies = pl.pallas_call(
        deliver,
        out_shape=(jax.ShapeDtypeStruct((1, TR, TC), f32), jax.ShapeDtypeStruct((SWEEPS, 1, COLOURS), f32)),
        in_specs=[vmem, vmem],
        out_specs=(anywhere, vmem),
        scratch_shapes=[dma((4,))],
        compiler_params=pltpu.CompilerParams(vmem_limit_bytes=VMEM_LIMIT),
        name="deliver",
    )(chunks, line)
    return final_field, energies.transpose(0, 2, 1)


def solution(mesh):
    placed = (
        P(None, "row", "col"),
        P("row", "col"),
        P("row", "col"),
        P("row", "col"),
        P("row", "col", None, None, None),
        P(),
    )
    return jax.shard_map(
        local, mesh=mesh, in_specs=placed, out_specs=(P(None, "row", "col"), P()), check_vma=False
    )
```

```python
import jax
import jax.numpy as jnp
from jax import lax
from jax.experimental import pallas as pl
from jax.experimental.pallas import tpu as pltpu
from jax.sharding import PartitionSpec as P

MESH = pl.DeviceIdType.MESH
SWEEPS = 2
COLOURS = 4
PHASES = SWEEPS * COLOURS
HALO = 16
TR = 128
TC = 512
EXT = TR + 2 * HALO
ROWS = EXT // 4
GROUPS = ROWS // 8
PAD = 8
PADDED = ROWS + 2 * PAD
LANES = 128
MIX = 73244475
VMEM_LIMIT = 32 * 1024 * 1024
STEP = 1.0 / 8388608.0
NODES = 8388608.0
DEVICES = 128
NEIGHBOURS = [(a, b) for a in (-1, 0, 1) for b in (-1, 0, 1) if (a, b) != (0, 0)]
LOWER = {(1, 0): 4, (2, 0): 5, (2, 1): 6, (3, 0): 7, (3, 1): 8, (3, 2): 9}
SINE = (6.283185307179586, -41.34170224039976, 81.60524927607506, -76.70585975306136, 42.05869394489765, -15.09464257682298, 3.8199525848482803)


def tile():
    return lax.broadcasted_iota(jnp.int32, (8, LANES), 0), lax.broadcasted_iota(jnp.int32, (8, LANES), 1)


def logical(value, amount):
    return lax.shift_right_logical(value, jnp.full_like(value, amount))


def scramble(hashed):
    hashed = (hashed ^ logical(hashed, 16)) * MIX
    hashed = (hashed ^ logical(hashed, 16)) * MIX
    return hashed ^ logical(hashed, 16)


def gaussian(base):
    one = (logical(scramble(base), 9).astype(jnp.float32) + 1.0) * STEP
    two = logical(scramble(base + 1), 9).astype(jnp.float32) * STEP
    squared = -2.0 * jnp.log(one)
    radius = squared * lax.rsqrt(jnp.maximum(squared, 1e-30))
    turn = jnp.abs(two - 0.5) - 0.25
    square = turn * turn
    series = jnp.full_like(square, SINE[6])
    for n in range(5, -1, -1):
        series = series * square + SINE[n]
    return radius * (turn * series)


def lane_next(main, side, lane):
    main, side = pltpu.roll(main, LANES - 1, 1), pltpu.roll(side, LANES - 1, 1)
    last = lane == LANES - 1
    return jnp.where(last, side, main), jnp.where(last, main, side)


def lane_prev(main, side, lane):
    main, side = pltpu.roll(main, 1, 1), pltpu.roll(side, 1, 1)
    first = lane == 0
    return jnp.where(first, side, main), jnp.where(first, main, side)


def pick(index, lane_source):
    return jnp.take_along_axis(lane_source, index, axis=1, mode="promise_in_bounds")


def kernel(
    field_ref, info_ref, kappa_ref, mass_ref, seed_ref, order_ref, outn, energy_ref,
    nat, halo, turned_nat, edge_planes, pack, strip_l, strip_r, seedbuf, seedmap, noise, fld, stf, inf, inv, scl, kd, fac, delta, acc, sums,
    load_sem, send_sem, recv_sem, esend, erecv, known,
):
    r, c = lax.axis_index("row"), lax.axis_index("col")
    sub, lane = tile()

    def at(dr, dc):
        return (lax.rem(r + (dr + 8), 8), lax.rem(c + (dc + 16), 16))

    barrier = pltpu.get_barrier_semaphore()
    peers = [at(*where) for where in NEIGHBOURS]
    peers += [at(0, k) for k in range(2, 15)] + [at(k, 0) for k in range(2, 7)]
    for peer in peers:
        pl.semaphore_signal(barrier, inc=1, device_id=peer, device_id_type=MESH)

    sources = (field_ref.at[0], info_ref, kappa_ref, mass_ref)
    loads = []
    for i in range(4):
        for k in range(4):
            loads.append(
                pltpu.make_async_copy(
                    sources[i].at[:, pl.ds(LANES * k, LANES)], nat.at[i, k, pl.ds(HALO, TR)], load_sem.at[i, k]
                )
            )
            loads[-1].start()

    own = jnp.zeros((8, LANES), jnp.int32)
    for t in range(SWEEPS):
        for colour in range(COLOURS):
            seed = jnp.int32(0)
            for k in range(COLOURS):
                seed = seed + jnp.where(order_ref[k] == colour, seed_ref[t, 0, k], 0)
            own = jnp.where(sub == t * COLOURS + colour, seed, own)
    seedbuf[4] = own

    for load in loads:
        load.wait()

    def pack_rows(g, _):
        rows = pl.ds(HALO + 8 * g, 8)
        total = jnp.zeros((8, LANES), jnp.float32)
        for i in range(4):
            right = pltpu.roll(nat[i, 3, rows, :], 16 * i + 16, 1)
            left = pltpu.roll(nat[i, 0, rows, :], 64 + 16 * i, 1)
            total = jnp.where((lane >= 16 * i) & (lane < 16 * i + 16), right, total)
            total = jnp.where((lane >= 64 + 16 * i) & (lane < 80 + 16 * i), left, total)
        pack[pl.ds(8 * g, 8), :] = total
        return 0

    lax.fori_loop(0, TR // 8, pack_rows, 0)

    pl.semaphore_wait(barrier, len(peers))
    copies = []

    def send(source, target, where):
        n = len(copies)
        copies.append(
            pltpu.make_async_remote_copy(
                src_ref=source,
                dst_ref=target,
                send_sem=send_sem.at[n],
                recv_sem=recv_sem.at[n],
                device_id=at(*where),
                device_id_type=MESH,
            )
        )
        copies[-1].start()

    for dr, dc in NEIGHBOURS:
        send(seedbuf.at[4], seedbuf.at[(1 - dr) * 3 + 1 - dc], (dr, dc))
    for dr in (-1, 0, 1):
        mine = {-1: pl.ds(0, HALO), 0: pl.ds(0, TR), 1: pl.ds(TR - HALO, HALO)}[dr]
        theirs = {-1: pl.ds(HALO + TR, HALO), 0: pl.ds(HALO, TR), 1: pl.ds(0, HALO)}[dr]
        send(pack.at[mine], strip_l.at[theirs], (dr, 1))
        send(pack.at[mine], strip_r.at[theirs], (dr, -1))
    send(nat.at[:, :, pl.ds(HALO, HALO)], halo.at[1, :, :, pl.ds(HALO, HALO)], (-1, 0))
    send(nat.at[:, :, pl.ds(TR, HALO)], halo.at[0, :, :, pl.ds(0, HALO)], (1, 0))
    for k in range(1, 8):
        pl.semaphore_signal(known, inc=1, device_id=at(k, 0), device_id_type=MESH)

    zero = jnp.zeros((8, LANES), jnp.float32)

    one = jnp.ones((8, LANES), jnp.float32)

    def clear(n, _):
        for i in range(4):
            nat[i, lax.rem(n, 4), pl.ds(pl.multiple_of(8 * (n // 4) + jnp.where(n >= 8, TR, 0), 8), 8), :] = one
        for v in range(2):
            for buffer in (fld, inv):
                buffer[n, v, 0:PAD, :] = zero
                buffer[n, v, PAD + ROWS : PADDED, :] = zero
            for i in range(PHASES):
                scl[i, n, v, 0:PAD, :] = zero
                scl[i, n, v, PAD + ROWS : PADDED, :] = zero
        return 0

    def clear_moves(i, _):
        for n in range(16):
            for v in range(2):
                kd[i, n, v, 0:PAD, :] = zero
                kd[i, n, v, PAD + ROWS : PADDED, :] = zero
                if n in (10, 11, 14, 15):
                    for g in range(GROUPS):
                        kd[i, n, v, PAD + 8 * g : PAD + 8 * g + 8, :] = zero
        return 0

    lax.fori_loop(0, PHASES - 1, clear_moves, 0)
    lax.fori_loop(0, 16, clear, 0)

    block = lane // 32
    split = [4 * (lane & 31) + ((block - k) & 3) for k in range(4)]
    edge = lane < 64
    used = (lane < 4) | (lane >= 124)

    def finish_planes(g, v):
        rows = pl.ds(8 * g, 8)
        padded = pl.ds(8 * g + PAD, 8)
        for n in range(16):
            mass = inv[n, v, padded, :]
            stf[n, v, rows, :] = stf[n, v, rows, :] * mass + 4.0
            inv[n, v, padded, :] = 1.0 / mass

    def place_of(g):
        rows, padded = pl.ds(8 * g, 8), pl.ds(8 * g + PAD, 8)
        return (fld, padded), (inf, rows), (stf, rows), (inv, padded)

    def gather_columns(g, load):
        for rho in range(4):
            for i in range(4):
                for k in range(4):
                    turned_nat[g, i, rho, k] = pick(split[k], load(i, k, rho))

    def turn_columns(g, part=None):
        for rho in range(4):
            for i, (ref, where) in enumerate(place_of(g)):
                chunks = [turned_nat[g, i, rho, k] for k in range(4)]
                for kappa in range(4):
                    m = chunks[(-kappa) & 3]
                    for b in range(1, 4):
                        m = jnp.where(block == b, chunks[(b - kappa) & 3], m)
                    m = pltpu.roll(m, LANES - 32 * kappa, 1) if kappa else m
                    if part is None:
                        ref[4 * rho + kappa, 0, where, :] = m
                    else:
                        edge_planes[i, 4 * rho + kappa, g // 4] = m

    def blend(g, part):
        rows, padded = pl.ds(8 * g, 8), pl.ds(8 * g + PAD, 8)
        for n in range(16):
            mass = edge_planes[3, n, g // 4]
            new = (edge_planes[0, n, g // 4], edge_planes[1, n, g // 4], edge_planes[2, n, g // 4] * mass + 4.0, 1.0 / mass)
            for ref, where, value in zip((fld, inf, stf, inv), (padded, rows, rows, padded), new):
                ref[n, 0, where, :] = jnp.where(part, value, ref[n, 0, where, :])

    def side_planes(g):
        for rho in range(4):
            natural = pl.ds(32 * g + rho, 8, stride=4)
            mixed = jnp.where(edge, strip_l[natural, :], strip_r[natural, :])
            for kappa in range(4):
                for i, (ref, where) in enumerate(place_of(g)):
                    index = 16 * i + 4 * (lane & 3) + kappa + jnp.where(edge, 64, 0)
                    ref[4 * rho + kappa, 1, where, :] = jnp.where(used, pick(index, mixed), 0.0 if i < 2 else 1.0)

    def draw(g, group_class, v):
        for rho in range(4):
            row = 4 * ((sub + (8 * g + 28)) & 31) + rho
            for kappa in range(4):
                colour = 2 * (rho // 2) + kappa // 2
                offset = 2 * (row * TC + 4 * lane + kappa)
                for t in range(SWEEPS):
                    seeds = seedmap[t * COLOURS + colour, v, group_class]
                    noise[t, 4 * rho + kappa, v, pl.ds(pl.multiple_of(8 * g, 8), 8), :] = gaussian(seeds + offset)

    def splat(slot, n):
        return jnp.broadcast_to(seedbuf[slot, n : n + 1, :], (8, LANES))

    for n in range(8):
        seedmap[n, 0, 1] = splat(4, n)

    def inner(g, _):
        draw(g, 1, 0)
        return 0

    lax.fori_loop(1, GROUPS - 1, inner, 0)

    for copy in copies[:8]:
        copy.wait()
    for n in range(8):
        seedmap[n, 0, 0] = jnp.where(sub < 4, splat(1, n), splat(4, n))
        seedmap[n, 0, 2] = jnp.where(sub < 4, splat(4, n), splat(7, n))
        rows = [jnp.where(lane < 64, splat(3 * a + 2, n), splat(3 * a, n)) for a in range(3)]
        seedmap[n, 1, 0] = jnp.where(sub < 4, rows[0], rows[1])
        seedmap[n, 1, 1] = rows[1]
        seedmap[n, 1, 2] = jnp.where(sub < 4, rows[1], rows[2])
    draw(0, 0, 0)
    draw(GROUPS - 1, 2, 0)

    def side(g, _):
        draw(g, jnp.where(g == 0, 0, jnp.where(g == GROUPS - 1, 2, 1)), 1)
        return 0

    lax.fori_loop(0, GROUPS, side, 0)

    for g in range(GROUPS):
        gather_columns(g, lambda i, k, rho, g=g: nat[i, k, pl.ds(32 * g + rho, 8, stride=4), :])
    for g in range(GROUPS):
        turn_columns(g)
    for g in range(GROUPS):
        finish_planes(g, 0)
    for copy in copies[8:14]:
        copy.wait()
    for g in range(GROUPS):
        side_planes(g)
    for g in range(GROUPS):
        finish_planes(g, 1)

    def around(ref, rho, kappa, base):
        up = (4 * ((rho + 3) % 4) + kappa, base - 1 if rho == 0 else base)
        down = (4 * ((rho + 1) % 4) + kappa, base + 1 if rho == 3 else base)
        here = pl.ds(base, 8)
        left = [ref[4 * rho + (kappa + 3) % 4, v, here, :] for v in range(2)]
        right = [ref[4 * rho + (kappa + 1) % 4, v, here, :] for v in range(2)]
        if kappa == 0:
            left = lane_prev(*left, lane)
        if kappa == 3:
            right = lane_next(*right, lane)
        return [
            ref[up[0], v, pl.ds(up[1], 8), :] + ref[down[0], v, pl.ds(down[1], 8), :] + left[v] + right[v]
            for v in range(2)
        ]

    def is_own(g):
        j = sub + 8 * g
        return (j >= 4) & (j < 36)

    def first(g, total):
        base = 8 * g + PAD
        rows = pl.ds(8 * g, 8)
        here = pl.ds(base, 8)
        part = zero
        for rho in range(4):
            for kappa in range(4):
                n = 4 * rho + kappa
                near = around(fld, rho, kappa, base)
                for v in range(2):
                    value = fld[n, v, here, :]
                    applied = stf[n, v, rows, :] * value - near[v]
                    scaled = inv[n, v, here, :] * applied
                    scl[0, n, v, here, :] = scaled
                    if v == 0:
                        part = part + (0.5 * scaled * applied - inf[n, v, rows, :] * value)
        return total + jnp.where(is_own(g), part, 0.0)


    def factors(g):
        base = 8 * g + PAD
        rows = pl.ds(8 * g, 8)
        here = pl.ds(base, 8)
        for colour in range(COLOURS):
            top, left = 2 * (colour // 2), 2 * (colour % 2)
            corner = [(top + n // 2, left + n % 2) for n in range(4)]
            near = [around(inv, rho, kappa, base) for rho, kappa in corner]
            for v in range(2):
                s = [stf[4 * rho + kappa, v, rows, :] for rho, kappa in corner]
                w = [inv[4 * rho + kappa, v, here, :] for rho, kappa in corner]
                sw = [s[n] * w[n] for n in range(4)]
                q = {(n, n): s[n] * sw[n] + near[n][v] for n in range(4)}
                for a, b in ((1, 0), (2, 0), (3, 1), (3, 2)):
                    q[a, b] = -(sw[a] + sw[b])
                q[3, 0] = w[1] + w[2]
                q[2, 1] = w[0] + w[3]
                low = {}
                for a in range(4):
                    for b in range(a + 1):
                        running = q[a, b]
                        for m in range(b):
                            running = running - low[a, m] * low[b, m]
                        low[a, b] = lax.rsqrt(running) if a == b else running * low[b, b]
                for n in range(4):
                    fac[n, colour, v, rows, :] = low[n, n]
                for (a, b), n in LOWER.items():
                    fac[n, colour, v, rows, :] = low[a, b]


    def resample(i, g, total, scatter):
        t, k = i // COLOURS, lax.rem(i, COLOURS)
        colour = order_ref[k]
        a, b = lax.shift_right_logical(colour, 1), colour & 1
        low_b = jnp.full((8, LANES), b, jnp.int32) == 0
        base = 8 * g + PAD
        rows = pl.ds(8 * g, 8)
        here = pl.ds(base, 8)
        rel_row = [2 * a, 2 * a + 1, (2 * a + 2) & 3, (2 * a + 3) & 3]
        rel_col = [2 * b, 2 * b + 1, (2 * b + 2) & 3, (2 * b + 3) & 3]
        above = pl.ds(base - jnp.where(a == 0, 1, 0), 8)
        below = pl.ds(base + jnp.where(a == 1, 1, 0), 8)

        def read(p, q, where=here):
            return [scl[i, 4 * rel_row[p] + rel_col[q], v, where, :] for v in range(2)]

        node = [[read(p, q) for q in range(2)] for p in range(2)]
        up = [read(3, q, above) for q in range(2)]
        down = [read(2, q, below) for q in range(2)]
        left, right = [], []
        for p in range(2):
            raw = read(p, 3)
            moved = lane_prev(*raw, lane)
            left.append([jnp.where(low_b, moved[v], raw[v]) for v in range(2)])
            raw = read(p, 2)
            moved = lane_next(*raw, lane)
            right.append([jnp.where(low_b, raw[v], moved[v]) for v in range(2)])
        moves = []
        for v in range(2):
            f, drawn = [], []
            inverse = [fac[n, colour, v, rows, :] for n in range(4)]
            low = {key: fac[n, colour, v, rows, :] for key, n in LOWER.items()}
            for n in range(4):
                p, q = n // 2, n % 2
                place = 4 * rel_row[p] + rel_col[q]
                near = node[1 - p][q][v] + node[p][1 - q][v]
                near = near + (down if p else up)[q][v] + (right if q else left)[p][v]
                running = inf[place, v, rows, :] - stf[place, v, rows, :] * node[p][q][v] + near
                for m in range(n):
                    running = running - low[n, m] * f[m]
                f.append(running * inverse[n])
                drawn.append(noise[t, place, v, rows, :])
            target = [f[n] + drawn[n] for n in range(4)]
            if v == 0 and scatter:
                part = (drawn[0] - f[0]) * target[0]
                for n in range(1, 4):
                    part = part + (drawn[n] - f[n]) * target[n]
                total = total + jnp.where(is_own(g), 0.5 * part, 0.0)
            move = [None] * 4
            for n in reversed(range(4)):
                running = target[n]
                for m in range(n + 1, 4):
                    running = running - low[m, n] * move[m]
                move[n] = running * inverse[n]
                if v == 0:
                    delta[i, n, rows, :] = move[n]
            if scatter:
                for n in range(4):
                    p, q = n // 2, n % 2
                    place = 4 * rel_row[p] + rel_col[q]
                    kd[i, 4 * p + q, v, here, :] = move[n ^ 1] + move[n ^ 2] - stf[place, v, rows, :] * move[n]
                for q in range(2):
                    kd[i, 12 + q, v, here, :] = move[q]
                    kd[i, 8 + q, v, here, :] = move[2 + q]
            moves.append(move)
        if scatter:
            for p in range(2):
                raw = [moves[v][2 * p] for v in range(2)]
                moved = lane_next(*raw, lane)
                for v in range(2):
                    kd[i, 4 * p + 3, v, here, :] = jnp.where(low_b, moved[v], raw[v])
                raw = [moves[v][2 * p + 1] for v in range(2)]
                moved = lane_prev(*raw, lane)
                for v in range(2):
                    kd[i, 4 * p + 2, v, here, :] = jnp.where(low_b, raw[v], moved[v])
        return total

    def spread(i, g):
        colour = order_ref[lax.rem(i, COLOURS)]
        a, b = lax.shift_right_logical(colour, 1), colour & 1
        base = 8 * g + PAD
        here = pl.ds(base, 8)
        for rho in range(4):
            where = here
            if rho == 3:
                where = pl.ds(base + jnp.where(a == 0, 1, 0), 8)
            if rho == 0:
                where = pl.ds(base - jnp.where(a == 1, 1, 0), 8)
            for kappa in range(4):
                n = 4 * rho + kappa
                place = 4 * ((rho + 4 - 2 * a) & 3) + ((kappa + 4 - 2 * b) & 3)
                for v in range(2):
                    scl[i + 1, n, v, here, :] = scl[i, n, v, here, :] - inv[n, v, here, :] * kd[i, place, v, where, :]

    inside, rim, every = range(1, GROUPS - 1), (0, GROUPS - 1), range(GROUPS)

    def phase(i, groups, counted):
        total = zero
        for g in groups:
            change = resample(i, g, zero, True)
            total = total + change if g in counted else total
        acc[i + 1] = total if counted is inside else acc[i + 1] + total
        for g in groups:
            spread(i, g)
        return 0

    total = zero
    for g in every:
        part = first(g, zero)
        total = total + part if g in inside else total
    acc[0] = total
    for g in every:
        factors(g)
    lax.fori_loop(0, PHASES - 1, lambda i, _: phase(i, every, inside), 0)
    for g in inside:
        resample(PHASES - 1, g, zero, False)

    for copy in copies[14:]:
        copy.wait()
    for g, side in ((0, 0), (GROUPS - 1, 1)):
        gather_columns(g, lambda i, k, rho, side=side: halo[side, i, k, pl.ds(rho, 8, stride=4), :])
    for g in rim:
        turn_columns(g, True)
    blend(0, sub < 4)
    blend(GROUPS - 1, sub >= 4)
    for g in rim:
        acc[0] = first(g, acc[0])
    for g in rim:
        factors(g)
    lax.fori_loop(0, PHASES - 1, lambda i, _: phase(i, rim, rim), 0)

    line = jnp.zeros((1, LANES), jnp.float32)
    for k in range(PHASES):
        change = jnp.sum(jnp.sum(acc[k], axis=0, keepdims=True), axis=1, keepdims=True)
        line = line + jnp.where(lane[0:1] >= k, change, 0.0)
    me = 16 * r + c
    mine = sums.at[pl.ds(me, 1)]
    sums[pl.ds(me, 1), :] = line
    pl.semaphore_wait(known, 7)

    def share(k, _):
        other = lax.rem(me + k, DEVICES)
        pltpu.make_async_remote_copy(
            src_ref=mine, dst_ref=mine, send_sem=esend, recv_sem=erecv,
            device_id=(other // 16, lax.rem(other, 16)), device_id_type=MESH,
        ).start()
        return 0

    lax.fori_loop(1, DEVICES, share, 0)

    for g in rim:
        resample(PHASES - 1, g, zero, False)

    turn_of = []
    for colour in range(COLOURS):
        turn = jnp.int32(0)
        for k in range(COLOURS):
            turn = jnp.where(order_ref[k] == colour, jnp.int32(k), turn)
        turn_of.append(turn)
    merge = [32 * (((lane & 3) + k) & 3) + lane // 4 for k in range(4)]

    def natural_rows(h, _):
        for rho in range(4):
            shifted = []
            for kappa in range(4):
                turn = turn_of[2 * (rho // 2) + kappa // 2]
                n = 2 * (rho % 2) + kappa % 2
                value = fld[4 * rho + kappa, 0, pl.ds(8 * h + PAD + 4, 8), :]
                value = value + delta[turn, n, pl.ds(8 * h + 4, 8), :]
                value = value + delta[turn + COLOURS, n, pl.ds(8 * h + 4, 8), :]
                shifted.append(pltpu.roll(value, 32 * kappa, 1) if kappa else value)
            for k in range(4):
                m = shifted[(-k) & 3]
                for b in range(1, 4):
                    m = jnp.where(block == b, shifted[(b - k) & 3], m)
                outn[k, pl.ds(32 * h + rho, 8, stride=4), :] = pick(merge[k], m)
        return 0

    lax.fori_loop(0, 4, natural_rows, 0)
    others = sums.at[pl.ds(0, DEVICES - 1)]
    pltpu.make_async_remote_copy(
        src_ref=others, dst_ref=others, send_sem=esend, recv_sem=erecv, device_id=at(0, 1), device_id_type=MESH
    ).wait()
    energy_ref[...] = jnp.broadcast_to(jnp.sum(sums[...], axis=0, keepdims=True) * (1.0 / NODES), (8, LANES))


def deliver(field_ref, energy_ref, out_ref, out_energy_ref, store_sem):
    stores = [
        pltpu.make_async_copy(field_ref.at[k], out_ref.at[0, :, pl.ds(LANES * k, LANES)], store_sem.at[k])
        for k in range(4)
    ]
    for store in stores:
        store.start()
    line = energy_ref[0:1, :]
    out_energy_ref[0] = line[:, 0:COLOURS]
    out_energy_ref[1] = pltpu.roll(line, LANES - COLOURS, 1)[:, 0:COLOURS]
    for store in stores:
        store.wait()


def local(initial_field, information, kappa_squared, lumped_mass, noise_seeds, colour_order):
    f32, i32 = jnp.float32, jnp.int32
    anywhere = pl.BlockSpec(memory_space=pltpu.HBM)
    scalar = pl.BlockSpec(memory_space=pltpu.SMEM)
    dma = pltpu.SemaphoreType.DMA
    seeds = noise_seeds.reshape(SWEEPS, COLOURS, 1).transpose(0, 2, 1)
    vmem = pl.BlockSpec(memory_space=pltpu.VMEM)
    arrays = (initial_field, information, kappa_squared, lumped_mass)
    chunks, line = pl.pallas_call(
        kernel,
        out_shape=(jax.ShapeDtypeStruct((4, TR, LANES), f32), jax.ShapeDtypeStruct((8, LANES), f32)),
        in_specs=[anywhere] * 4 + [scalar] * 2,
        out_specs=(vmem, vmem),
        scratch_shapes=[
            pltpu.VMEM((4, 4, EXT, LANES), f32),
            pltpu.VMEM((2, 4, 4, 2 * HALO, LANES), f32),
            pltpu.VMEM((GROUPS, 4, 4, 4, 8, LANES), f32),
            pltpu.VMEM((4, 16, 2, 8, LANES), f32),
            pltpu.VMEM((TR, LANES), f32),
            pltpu.VMEM((EXT, LANES), f32),
            pltpu.VMEM((EXT, LANES), f32),
            pltpu.VMEM((9, 8, LANES), i32),
            pltpu.VMEM((8, 2, 3, 8, LANES), i32),
            pltpu.VMEM((SWEEPS, 16, 2, ROWS, LANES), f32),
            pltpu.VMEM((16, 2, PADDED, LANES), f32),
            pltpu.VMEM((16, 2, ROWS, LANES), f32),
            pltpu.VMEM((16, 2, ROWS, LANES), f32),
            pltpu.VMEM((16, 2, PADDED, LANES), f32),
            pltpu.VMEM((PHASES, 16, 2, PADDED, LANES), f32),
            pltpu.VMEM((PHASES - 1, 16, 2, PADDED, LANES), f32),
            pltpu.VMEM((10, COLOURS, 2, ROWS, LANES), f32),
            pltpu.VMEM((PHASES, 4, ROWS, LANES), f32),
            pltpu.VMEM((PHASES, 8, LANES), f32),
            pltpu.VMEM((DEVICES, LANES), f32),
            dma((4, 4)),
            dma((16,)),
            dma((16,)),
            dma,
            dma,
            pltpu.SemaphoreType.REGULAR,
        ],
        compiler_params=pltpu.CompilerParams(collective_id=0, has_side_effects=True, vmem_limit_bytes=VMEM_LIMIT),
        name="gibbs",
    )(*(pltpu.with_memory_space_constraint(a, pltpu.HBM) for a in (*arrays, seeds, colour_order)))
    final_field, energies = pl.pallas_call(
        deliver,
        out_shape=(jax.ShapeDtypeStruct((1, TR, TC), f32), jax.ShapeDtypeStruct((SWEEPS, 1, COLOURS), f32)),
        in_specs=[vmem, vmem],
        out_specs=(anywhere, vmem),
        scratch_shapes=[dma((4,))],
        compiler_params=pltpu.CompilerParams(vmem_limit_bytes=VMEM_LIMIT),
        name="deliver",
    )(chunks, line)
    return final_field, energies.transpose(0, 2, 1)


def solution(mesh):
    placed = (
        P(None, "row", "col"),
        P("row", "col"),
        P("row", "col"),
        P("row", "col"),
        P("row", "col", None, None, None),
        P(),
    )
    return jax.shard_map(
        local, mesh=mesh, in_specs=placed, out_specs=(P(None, "row", "col"), P()), check_vma=False
    )
```

```python
import jax
import jax.numpy as jnp
from jax import lax
from jax.experimental import pallas as pl
from jax.experimental.pallas import tpu as pltpu
from jax.sharding import PartitionSpec as P

MESH = pl.DeviceIdType.MESH
SWEEPS = 2
COLOURS = 4
PHASES = SWEEPS * COLOURS
HALO = 16
TR = 128
TC = 512
EXT = TR + 2 * HALO
ROWS = EXT // 4
GROUPS = ROWS // 8
PAD = 8
PADDED = ROWS + 2 * PAD
LANES = 128
MIX = 73244475
VMEM_LIMIT = 32 * 1024 * 1024
STEP = 1.0 / 8388608.0
NODES = 8388608.0
DEVICES = 128
NEIGHBOURS = [(a, b) for a in (-1, 0, 1) for b in (-1, 0, 1) if (a, b) != (0, 0)]
LOWER = {(1, 0): 4, (2, 0): 5, (2, 1): 6, (3, 0): 7, (3, 1): 8, (3, 2): 9}
SINE = (6.283185307179586, -41.34170224039976, 81.60524927607506, -76.70585975306136, 42.05869394489765, -15.09464257682298, 3.8199525848482803)


def tile():
    return lax.broadcasted_iota(jnp.int32, (8, LANES), 0), lax.broadcasted_iota(jnp.int32, (8, LANES), 1)


def logical(value, amount):
    return lax.shift_right_logical(value, jnp.full_like(value, amount))


def scramble(hashed):
    hashed = (hashed ^ logical(hashed, 16)) * MIX
    hashed = (hashed ^ logical(hashed, 16)) * MIX
    return hashed ^ logical(hashed, 16)


def gaussian(base):
    one = (logical(scramble(base), 9).astype(jnp.float32) + 1.0) * STEP
    two = logical(scramble(base + 1), 9).astype(jnp.float32) * STEP
    squared = -2.0 * jnp.log(one)
    radius = squared * lax.rsqrt(jnp.maximum(squared, 1e-30))
    turn = jnp.abs(two - 0.5) - 0.25
    square = turn * turn
    series = jnp.full_like(square, SINE[6])
    for n in range(5, -1, -1):
        series = series * square + SINE[n]
    return radius * (turn * series)


def lane_next(main, side, lane):
    main, side = pltpu.roll(main, LANES - 1, 1), pltpu.roll(side, LANES - 1, 1)
    last = lane == LANES - 1
    return jnp.where(last, side, main), jnp.where(last, main, side)


def lane_prev(main, side, lane):
    main, side = pltpu.roll(main, 1, 1), pltpu.roll(side, 1, 1)
    first = lane == 0
    return jnp.where(first, side, main), jnp.where(first, main, side)


def pick(index, lane_source):
    return jnp.take_along_axis(lane_source, index, axis=1, mode="promise_in_bounds")


def kernel(
    field_ref, info_ref, kappa_ref, mass_ref, seed_ref, order_ref, outn, energy_ref,
    nat, halo, turned_nat, edge_planes, pack, strip_l, strip_r, seedbuf, seedmap, noise, fld, stf, inf, inv, scl, kd, fac, delta, acc, sums,
    load_sem, send_sem, recv_sem, esend, erecv, known,
):
    r, c = lax.axis_index("row"), lax.axis_index("col")
    sub, lane = tile()

    def at(dr, dc):
        return (lax.rem(r + (dr + 8), 8), lax.rem(c + (dc + 16), 16))

    barrier = pltpu.get_barrier_semaphore()
    peers = [at(*where) for where in NEIGHBOURS]
    peers += [at(0, k) for k in range(2, 15)] + [at(k, 0) for k in range(2, 7)]
    for peer in peers[:8]:
        pl.semaphore_signal(barrier, inc=1, device_id=peer, device_id_type=MESH)

    sources = (field_ref.at[0], info_ref, kappa_ref, mass_ref)
    loads = []
    for i in range(4):
        for k in range(4):
            loads.append(
                pltpu.make_async_copy(
                    sources[i].at[:, pl.ds(LANES * k, LANES)], nat.at[i, k, pl.ds(HALO, TR)], load_sem.at[i, k]
                )
            )
            loads[-1].start()

    for peer in peers[8:]:
        pl.semaphore_signal(barrier, inc=1, device_id=peer, device_id_type=MESH)

    own = jnp.zeros((8, LANES), jnp.int32)
    for t in range(SWEEPS):
        for colour in range(COLOURS):
            seed = jnp.int32(0)
            for k in range(COLOURS):
                seed = seed + jnp.where(order_ref[k] == colour, seed_ref[t, 0, k], 0)
            own = jnp.where(sub == t * COLOURS + colour, seed, own)
    seedbuf[4] = own

    pl.semaphore_wait(barrier, len(peers))
    copies = []

    def send(source, target, where):
        n = len(copies)
        copies.append(
            pltpu.make_async_remote_copy(
                src_ref=source,
                dst_ref=target,
                send_sem=send_sem.at[n],
                recv_sem=recv_sem.at[n],
                device_id=at(*where),
                device_id_type=MESH,
            )
        )
        copies[-1].start()

    for dr, dc in NEIGHBOURS:
        send(seedbuf.at[4], seedbuf.at[(1 - dr) * 3 + 1 - dc], (dr, dc))
    for load in loads:
        load.wait()
    for g in range(TR // 8):
        rows = pl.ds(HALO + 8 * g, 8)
        total = jnp.zeros((8, LANES), jnp.float32)
        for i in range(4):
            right = pltpu.roll(nat[i, 3, rows, :], 16 * i + 16, 1)
            left = pltpu.roll(nat[i, 0, rows, :], 64 + 16 * i, 1)
            total = jnp.where((lane >= 16 * i) & (lane < 16 * i + 16), right, total)
            total = jnp.where((lane >= 64 + 16 * i) & (lane < 80 + 16 * i), left, total)
        pack[pl.ds(8 * g, 8), :] = total
    def splat(slot, n):
        return jnp.broadcast_to(seedbuf[slot, n : n + 1, :], (8, LANES))

    for n in range(8):
        seedmap[n, 0, 1] = splat(4, n)
    for dr in (-1, 0, 1):
        mine = {-1: pl.ds(0, HALO), 0: pl.ds(0, TR), 1: pl.ds(TR - HALO, HALO)}[dr]
        theirs = {-1: pl.ds(HALO + TR, HALO), 0: pl.ds(HALO, TR), 1: pl.ds(0, HALO)}[dr]
        send(pack.at[mine], strip_l.at[theirs], (dr, 1))
        send(pack.at[mine], strip_r.at[theirs], (dr, -1))
    send(nat.at[:, :, pl.ds(HALO, HALO)], halo.at[1, :, :, pl.ds(HALO, HALO)], (-1, 0))
    send(nat.at[:, :, pl.ds(TR, HALO)], halo.at[0, :, :, pl.ds(0, HALO)], (1, 0))
    for k in range(1, 8):
        pl.semaphore_signal(known, inc=1, device_id=at(k, 0), device_id_type=MESH)

    zero = jnp.zeros((8, LANES), jnp.float32)

    one = jnp.ones((8, LANES), jnp.float32)

    def clear(n, _):
        for i in range(4):
            nat[i, lax.rem(n, 4), pl.ds(pl.multiple_of(8 * (n // 4) + jnp.where(n >= 8, TR, 0), 8), 8), :] = one
        for v in range(2):
            for buffer in (fld, inv):
                buffer[n, v, 0:PAD, :] = zero
                buffer[n, v, PAD + ROWS : PADDED, :] = zero
            for i in range(PHASES):
                scl[i, n, v, 0:PAD, :] = zero
                scl[i, n, v, PAD + ROWS : PADDED, :] = zero
        return 0

    def clear_moves(i, _):
        for n in range(16):
            for v in range(2):
                kd[i, n, v, 0:PAD, :] = zero
                kd[i, n, v, PAD + ROWS : PADDED, :] = zero
                if n in (10, 11, 14, 15):
                    for g in range(GROUPS):
                        kd[i, n, v, PAD + 8 * g : PAD + 8 * g + 8, :] = zero
        return 0

    lax.fori_loop(0, PHASES - 1, clear_moves, 0)
    lax.fori_loop(0, 16, clear, 0)

    block = lane // 32
    split = [4 * (lane & 31) + ((block - k) & 3) for k in range(4)]
    edge = lane < 64
    used = (lane < 4) | (lane >= 124)

    def finish_planes(g, v):
        rows = pl.ds(8 * g, 8)
        padded = pl.ds(8 * g + PAD, 8)
        for n in range(16):
            mass = inv[n, v, padded, :]
            stf[n, v, rows, :] = stf[n, v, rows, :] * mass + 4.0
            inv[n, v, padded, :] = 1.0 / mass

    def place_of(g):
        rows, padded = pl.ds(8 * g, 8), pl.ds(8 * g + PAD, 8)
        return (fld, padded), (inf, rows), (stf, rows), (inv, padded)

    def gather_columns(g, load):
        for rho in range(4):
            for i in range(4):
                for k in range(4):
                    turned_nat[g, i, rho, k] = pick(split[k], load(i, k, rho))

    def turn_columns(g, part=None):
        for rho in range(4):
            for i, (ref, where) in enumerate(place_of(g)):
                chunks = [turned_nat[g, i, rho, k] for k in range(4)]
                for kappa in range(4):
                    m = chunks[(-kappa) & 3]
                    for b in range(1, 4):
                        m = jnp.where(block == b, chunks[(b - kappa) & 3], m)
                    m = pltpu.roll(m, LANES - 32 * kappa, 1) if kappa else m
                    if part is None:
                        ref[4 * rho + kappa, 0, where, :] = m
                    else:
                        edge_planes[i, 4 * rho + kappa, g // 4] = m

    def blend(g, part):
        rows, padded = pl.ds(8 * g, 8), pl.ds(8 * g + PAD, 8)
        for n in range(16):
            mass = edge_planes[3, n, g // 4]
            new = (edge_planes[0, n, g // 4], edge_planes[1, n, g // 4], edge_planes[2, n, g // 4] * mass + 4.0, 1.0 / mass)
            for ref, where, value in zip((fld, inf, stf, inv), (padded, rows, rows, padded), new):
                ref[n, 0, where, :] = jnp.where(part, value, ref[n, 0, where, :])

    def side_planes(g):
        for rho in range(4):
            natural = pl.ds(32 * g + rho, 8, stride=4)
            mixed = jnp.where(edge, strip_l[natural, :], strip_r[natural, :])
            for kappa in range(4):
                for i, (ref, where) in enumerate(place_of(g)):
                    index = 16 * i + 4 * (lane & 3) + kappa + jnp.where(edge, 64, 0)
                    ref[4 * rho + kappa, 1, where, :] = jnp.where(used, pick(index, mixed), 0.0 if i < 2 else 1.0)

    def draw(g, group_class, v):
        for rho in range(4):
            row = 4 * ((sub + (8 * g + 28)) & 31) + rho
            for kappa in range(4):
                colour = 2 * (rho // 2) + kappa // 2
                offset = 2 * (row * TC + 4 * lane + kappa)
                for t in range(SWEEPS):
                    seeds = seedmap[t * COLOURS + colour, v, group_class]
                    noise[t, 4 * rho + kappa, v, pl.ds(pl.multiple_of(8 * g, 8), 8), :] = gaussian(seeds + offset)

    def inner(g, _):
        draw(g, 1, 0)
        return 0

    lax.fori_loop(1, GROUPS - 1, inner, 0)

    for g in range(GROUPS):
        gather_columns(g, lambda i, k, rho, g=g: nat[i, k, pl.ds(32 * g + rho, 8, stride=4), :])
    for g in range(GROUPS):
        turn_columns(g)
    for g in range(GROUPS):
        finish_planes(g, 0)
    for copy in copies[:8]:
        copy.wait()
    for n in range(8):
        seedmap[n, 0, 0] = jnp.where(sub < 4, splat(1, n), splat(4, n))
        seedmap[n, 0, 2] = jnp.where(sub < 4, splat(4, n), splat(7, n))
        rows = [jnp.where(lane < 64, splat(3 * a + 2, n), splat(3 * a, n)) for a in range(3)]
        seedmap[n, 1, 0] = jnp.where(sub < 4, rows[0], rows[1])
        seedmap[n, 1, 1] = rows[1]
        seedmap[n, 1, 2] = jnp.where(sub < 4, rows[1], rows[2])
    draw(0, 0, 0)
    draw(GROUPS - 1, 2, 0)

    def side(g, _):
        draw(g, jnp.where(g == 0, 0, jnp.where(g == GROUPS - 1, 2, 1)), 1)
        return 0

    lax.fori_loop(0, GROUPS, side, 0)

    for copy in copies[8:14]:
        copy.wait()
    for g in range(GROUPS):
        side_planes(g)
    for g in range(GROUPS):
        finish_planes(g, 1)

    def around(ref, rho, kappa, base):
        up = (4 * ((rho + 3) % 4) + kappa, base - 1 if rho == 0 else base)
        down = (4 * ((rho + 1) % 4) + kappa, base + 1 if rho == 3 else base)
        here = pl.ds(base, 8)
        left = [ref[4 * rho + (kappa + 3) % 4, v, here, :] for v in range(2)]
        right = [ref[4 * rho + (kappa + 1) % 4, v, here, :] for v in range(2)]
        if kappa == 0:
            left = lane_prev(*left, lane)
        if kappa == 3:
            right = lane_next(*right, lane)
        return [
            ref[up[0], v, pl.ds(up[1], 8), :] + ref[down[0], v, pl.ds(down[1], 8), :] + left[v] + right[v]
            for v in range(2)
        ]

    def is_own(g):
        j = sub + 8 * g
        return (j >= 4) & (j < 36)

    def first(g, total):
        base = 8 * g + PAD
        rows = pl.ds(8 * g, 8)
        here = pl.ds(base, 8)
        part = zero
        for rho in range(4):
            for kappa in range(4):
                n = 4 * rho + kappa
                near = around(fld, rho, kappa, base)
                for v in range(2):
                    value = fld[n, v, here, :]
                    applied = stf[n, v, rows, :] * value - near[v]
                    scaled = inv[n, v, here, :] * applied
                    scl[0, n, v, here, :] = scaled
                    if v == 0:
                        part = part + (0.5 * scaled * applied - inf[n, v, rows, :] * value)
        return total + jnp.where(is_own(g), part, 0.0)


    def factors(g):
        base = 8 * g + PAD
        rows = pl.ds(8 * g, 8)
        here = pl.ds(base, 8)
        for colour in range(COLOURS):
            top, left = 2 * (colour // 2), 2 * (colour % 2)
            corner = [(top + n // 2, left + n % 2) for n in range(4)]
            near = [around(inv, rho, kappa, base) for rho, kappa in corner]
            for v in range(2):
                s = [stf[4 * rho + kappa, v, rows, :] for rho, kappa in corner]
                w = [inv[4 * rho + kappa, v, here, :] for rho, kappa in corner]
                sw = [s[n] * w[n] for n in range(4)]
                q = {(n, n): s[n] * sw[n] + near[n][v] for n in range(4)}
                for a, b in ((1, 0), (2, 0), (3, 1), (3, 2)):
                    q[a, b] = -(sw[a] + sw[b])
                q[3, 0] = w[1] + w[2]
                q[2, 1] = w[0] + w[3]
                low = {}
                for a in range(4):
                    for b in range(a + 1):
                        running = q[a, b]
                        for m in range(b):
                            running = running - low[a, m] * low[b, m]
                        low[a, b] = lax.rsqrt(running) if a == b else running * low[b, b]
                for n in range(4):
                    fac[n, colour, v, rows, :] = low[n, n]
                for (a, b), n in LOWER.items():
                    fac[n, colour, v, rows, :] = low[a, b]


    def resample(i, g, total, scatter):
        t, k = i // COLOURS, lax.rem(i, COLOURS)
        colour = order_ref[k]
        a, b = lax.shift_right_logical(colour, 1), colour & 1
        low_b = jnp.full((8, LANES), b, jnp.int32) == 0
        base = 8 * g + PAD
        rows = pl.ds(8 * g, 8)
        here = pl.ds(base, 8)
        rel_row = [2 * a, 2 * a + 1, (2 * a + 2) & 3, (2 * a + 3) & 3]
        rel_col = [2 * b, 2 * b + 1, (2 * b + 2) & 3, (2 * b + 3) & 3]
        above = pl.ds(base - jnp.where(a == 0, 1, 0), 8)
        below = pl.ds(base + jnp.where(a == 1, 1, 0), 8)

        def read(p, q, where=here):
            return [scl[i, 4 * rel_row[p] + rel_col[q], v, where, :] for v in range(2)]

        node = [[read(p, q) for q in range(2)] for p in range(2)]
        up = [read(3, q, above) for q in range(2)]
        down = [read(2, q, below) for q in range(2)]
        left, right = [], []
        for p in range(2):
            raw = read(p, 3)
            moved = lane_prev(*raw, lane)
            left.append([jnp.where(low_b, moved[v], raw[v]) for v in range(2)])
            raw = read(p, 2)
            moved = lane_next(*raw, lane)
            right.append([jnp.where(low_b, raw[v], moved[v]) for v in range(2)])
        moves = []
        for v in range(2):
            f, drawn = [], []
            inverse = [fac[n, colour, v, rows, :] for n in range(4)]
            low = {key: fac[n, colour, v, rows, :] for key, n in LOWER.items()}
            for n in range(4):
                p, q = n // 2, n % 2
                place = 4 * rel_row[p] + rel_col[q]
                near = node[1 - p][q][v] + node[p][1 - q][v]
                near = near + (down if p else up)[q][v] + (right if q else left)[p][v]
                running = inf[place, v, rows, :] - stf[place, v, rows, :] * node[p][q][v] + near
                for m in range(n):
                    running = running - low[n, m] * f[m]
                f.append(running * inverse[n])
                drawn.append(noise[t, place, v, rows, :])
            target = [f[n] + drawn[n] for n in range(4)]
            if v == 0 and scatter:
                part = (drawn[0] - f[0]) * target[0]
                for n in range(1, 4):
                    part = part + (drawn[n] - f[n]) * target[n]
                total = total + jnp.where(is_own(g), 0.5 * part, 0.0)
            move = [None] * 4
            for n in reversed(range(4)):
                running = target[n]
                for m in range(n + 1, 4):
                    running = running - low[m, n] * move[m]
                move[n] = running * inverse[n]
                if v == 0:
                    delta[i, n, rows, :] = move[n]
            if scatter:
                for n in range(4):
                    p, q = n // 2, n % 2
                    place = 4 * rel_row[p] + rel_col[q]
                    kd[i, 4 * p + q, v, here, :] = move[n ^ 1] + move[n ^ 2] - stf[place, v, rows, :] * move[n]
                for q in range(2):
                    kd[i, 12 + q, v, here, :] = move[q]
                    kd[i, 8 + q, v, here, :] = move[2 + q]
            moves.append(move)
        if scatter:
            for p in range(2):
                raw = [moves[v][2 * p] for v in range(2)]
                moved = lane_next(*raw, lane)
                for v in range(2):
                    kd[i, 4 * p + 3, v, here, :] = jnp.where(low_b, moved[v], raw[v])
                raw = [moves[v][2 * p + 1] for v in range(2)]
                moved = lane_prev(*raw, lane)
                for v in range(2):
                    kd[i, 4 * p + 2, v, here, :] = jnp.where(low_b, raw[v], moved[v])
        return total

    def spread(i, g):
        colour = order_ref[lax.rem(i, COLOURS)]
        a, b = lax.shift_right_logical(colour, 1), colour & 1
        base = 8 * g + PAD
        here = pl.ds(base, 8)
        for rho in range(4):
            where = here
            if rho == 3:
                where = pl.ds(base + jnp.where(a == 0, 1, 0), 8)
            if rho == 0:
                where = pl.ds(base - jnp.where(a == 1, 1, 0), 8)
            for kappa in range(4):
                n = 4 * rho + kappa
                place = 4 * ((rho + 4 - 2 * a) & 3) + ((kappa + 4 - 2 * b) & 3)
                for v in range(2):
                    scl[i + 1, n, v, here, :] = scl[i, n, v, here, :] - inv[n, v, here, :] * kd[i, place, v, where, :]

    inside, rim, every = range(1, GROUPS - 1), (0, GROUPS - 1), range(GROUPS)

    def phase(i, groups, counted):
        total = zero
        for g in groups:
            change = resample(i, g, zero, True)
            total = total + change if g in counted else total
        acc[i + 1] = total if counted is inside else acc[i + 1] + total
        for g in groups:
            spread(i, g)
        return 0

    total = zero
    for g in every:
        part = first(g, zero)
        total = total + part if g in inside else total
    acc[0] = total
    for g in every:
        factors(g)
    lax.fori_loop(0, PHASES - 1, lambda i, _: phase(i, every, inside), 0)
    for g in inside:
        resample(PHASES - 1, g, zero, False)

    for copy in copies[14:]:
        copy.wait()
    for g, side in ((0, 0), (GROUPS - 1, 1)):
        gather_columns(g, lambda i, k, rho, side=side: halo[side, i, k, pl.ds(rho, 8, stride=4), :])
    for g in rim:
        turn_columns(g, True)
    blend(0, sub < 4)
    blend(GROUPS - 1, sub >= 4)
    for g in rim:
        acc[0] = first(g, acc[0])
    for g in rim:
        factors(g)
    lax.fori_loop(0, PHASES - 1, lambda i, _: phase(i, rim, rim), 0)

    line = jnp.zeros((1, LANES), jnp.float32)
    for k in range(PHASES):
        change = jnp.sum(jnp.sum(acc[k], axis=0, keepdims=True), axis=1, keepdims=True)
        line = line + jnp.where(lane[0:1] >= k, change, 0.0)
    me = 16 * r + c
    mine = sums.at[pl.ds(me, 1)]
    sums[pl.ds(me, 1), :] = line
    pl.semaphore_wait(known, 7)

    def share(k, _):
        other = lax.rem(me + k, DEVICES)
        pltpu.make_async_remote_copy(
            src_ref=mine, dst_ref=mine, send_sem=esend, recv_sem=erecv,
            device_id=(other // 16, lax.rem(other, 16)), device_id_type=MESH,
        ).start()
        return 0

    lax.fori_loop(1, DEVICES, share, 0)

    for g in rim:
        resample(PHASES - 1, g, zero, False)

    turn_of = []
    for colour in range(COLOURS):
        turn = jnp.int32(0)
        for k in range(COLOURS):
            turn = jnp.where(order_ref[k] == colour, jnp.int32(k), turn)
        turn_of.append(turn)
    merge = [32 * (((lane & 3) + k) & 3) + lane // 4 for k in range(4)]

    def natural_rows(h, _):
        for rho in range(4):
            shifted = []
            for kappa in range(4):
                turn = turn_of[2 * (rho // 2) + kappa // 2]
                n = 2 * (rho % 2) + kappa % 2
                value = fld[4 * rho + kappa, 0, pl.ds(8 * h + PAD + 4, 8), :]
                value = value + delta[turn, n, pl.ds(8 * h + 4, 8), :]
                value = value + delta[turn + COLOURS, n, pl.ds(8 * h + 4, 8), :]
                shifted.append(pltpu.roll(value, 32 * kappa, 1) if kappa else value)
            for k in range(4):
                m = shifted[(-k) & 3]
                for b in range(1, 4):
                    m = jnp.where(block == b, shifted[(b - k) & 3], m)
                outn[k, pl.ds(32 * h + rho, 8, stride=4), :] = pick(merge[k], m)
        return 0

    lax.fori_loop(0, 4, natural_rows, 0)
    others = sums.at[pl.ds(0, DEVICES - 1)]
    pltpu.make_async_remote_copy(
        src_ref=others, dst_ref=others, send_sem=esend, recv_sem=erecv, device_id=at(0, 1), device_id_type=MESH
    ).wait()
    energy_ref[...] = jnp.broadcast_to(jnp.sum(sums[...], axis=0, keepdims=True) * (1.0 / NODES), (8, LANES))


def deliver(field_ref, energy_ref, out_ref, out_energy_ref, store_sem):
    stores = [
        pltpu.make_async_copy(field_ref.at[k], out_ref.at[0, :, pl.ds(LANES * k, LANES)], store_sem.at[k])
        for k in range(4)
    ]
    for store in stores:
        store.start()
    line = energy_ref[0:1, :]
    out_energy_ref[0] = line[:, 0:COLOURS]
    out_energy_ref[1] = pltpu.roll(line, LANES - COLOURS, 1)[:, 0:COLOURS]
    for store in stores:
        store.wait()


def local(initial_field, information, kappa_squared, lumped_mass, noise_seeds, colour_order):
    f32, i32 = jnp.float32, jnp.int32
    anywhere = pl.BlockSpec(memory_space=pltpu.HBM)
    scalar = pl.BlockSpec(memory_space=pltpu.SMEM)
    dma = pltpu.SemaphoreType.DMA
    seeds = noise_seeds.reshape(SWEEPS, COLOURS, 1).transpose(0, 2, 1)
    vmem = pl.BlockSpec(memory_space=pltpu.VMEM)
    arrays = (initial_field, information, kappa_squared, lumped_mass)
    chunks, line = pl.pallas_call(
        kernel,
        out_shape=(jax.ShapeDtypeStruct((4, TR, LANES), f32), jax.ShapeDtypeStruct((8, LANES), f32)),
        in_specs=[anywhere] * 4 + [scalar] * 2,
        out_specs=(vmem, vmem),
        scratch_shapes=[
            pltpu.VMEM((4, 4, EXT, LANES), f32),
            pltpu.VMEM((2, 4, 4, 2 * HALO, LANES), f32),
            pltpu.VMEM((GROUPS, 4, 4, 4, 8, LANES), f32),
            pltpu.VMEM((4, 16, 2, 8, LANES), f32),
            pltpu.VMEM((TR, LANES), f32),
            pltpu.VMEM((EXT, LANES), f32),
            pltpu.VMEM((EXT, LANES), f32),
            pltpu.VMEM((9, 8, LANES), i32),
            pltpu.VMEM((8, 2, 3, 8, LANES), i32),
            pltpu.VMEM((SWEEPS, 16, 2, ROWS, LANES), f32),
            pltpu.VMEM((16, 2, PADDED, LANES), f32),
            pltpu.VMEM((16, 2, ROWS, LANES), f32),
            pltpu.VMEM((16, 2, ROWS, LANES), f32),
            pltpu.VMEM((16, 2, PADDED, LANES), f32),
            pltpu.VMEM((PHASES, 16, 2, PADDED, LANES), f32),
            pltpu.VMEM((PHASES - 1, 16, 2, PADDED, LANES), f32),
            pltpu.VMEM((10, COLOURS, 2, ROWS, LANES), f32),
            pltpu.VMEM((PHASES, 4, ROWS, LANES), f32),
            pltpu.VMEM((PHASES, 8, LANES), f32),
            pltpu.VMEM((DEVICES, LANES), f32),
            dma((4, 4)),
            dma((16,)),
            dma((16,)),
            dma,
            dma,
            pltpu.SemaphoreType.REGULAR,
        ],
        compiler_params=pltpu.CompilerParams(collective_id=0, has_side_effects=True, vmem_limit_bytes=VMEM_LIMIT),
        name="gibbs",
    )(*(pltpu.with_memory_space_constraint(a, pltpu.HBM) for a in (*arrays, seeds, colour_order)))
    final_field, energies = pl.pallas_call(
        deliver,
        out_shape=(jax.ShapeDtypeStruct((1, TR, TC), f32), jax.ShapeDtypeStruct((SWEEPS, 1, COLOURS), f32)),
        in_specs=[vmem, vmem],
        out_specs=(anywhere, vmem),
        scratch_shapes=[dma((4,))],
        compiler_params=pltpu.CompilerParams(vmem_limit_bytes=VMEM_LIMIT),
        name="deliver",
    )(chunks, line)
    return final_field, energies.transpose(0, 2, 1)


def solution(mesh):
    placed = (
        P(None, "row", "col"),
        P("row", "col"),
        P("row", "col"),
        P("row", "col"),
        P("row", "col", None, None, None),
        P(),
    )
    return jax.shard_map(
        local, mesh=mesh, in_specs=placed, out_specs=(P(None, "row", "col"), P()), check_vma=False
    )
```

```python
import jax
import jax.numpy as jnp
from jax import lax
from jax.experimental import pallas as pl
from jax.experimental.pallas import tpu as pltpu
from jax.sharding import PartitionSpec as P

MESH = pl.DeviceIdType.MESH
SWEEPS = 2
COLOURS = 4
PHASES = SWEEPS * COLOURS
HALO = 16
TR = 128
TC = 512
EXT = TR + 2 * HALO
ROWS = EXT // 4
GROUPS = ROWS // 8
PAD = 8
PADDED = ROWS + 2 * PAD
LANES = 128
MIX = 73244475
VMEM_LIMIT = 32 * 1024 * 1024
STEP = 1.0 / 8388608.0
NODES = 8388608.0
DEVICES = 128
NEIGHBOURS = [(a, b) for a in (-1, 0, 1) for b in (-1, 0, 1) if (a, b) != (0, 0)]
LOWER = {(1, 0): 4, (2, 0): 5, (2, 1): 6, (3, 0): 7, (3, 1): 8, (3, 2): 9}
SINE = (6.283185307179586, -41.34170224039976, 81.60524927607506, -76.70585975306136, 42.05869394489765, -15.09464257682298, 3.8199525848482803)


def tile():
    return lax.broadcasted_iota(jnp.int32, (8, LANES), 0), lax.broadcasted_iota(jnp.int32, (8, LANES), 1)


def logical(value, amount):
    return lax.shift_right_logical(value, jnp.full_like(value, amount))


def scramble(hashed):
    hashed = (hashed ^ logical(hashed, 16)) * MIX
    hashed = (hashed ^ logical(hashed, 16)) * MIX
    return hashed ^ logical(hashed, 16)


def gaussian(base):
    one = (logical(scramble(base), 9).astype(jnp.float32) + 1.0) * STEP
    two = logical(scramble(base + 1), 9).astype(jnp.float32) * STEP
    squared = -2.0 * jnp.log(one)
    radius = squared * lax.rsqrt(jnp.maximum(squared, 1e-30))
    turn = jnp.abs(two - 0.5) - 0.25
    square = turn * turn
    series = jnp.full_like(square, SINE[6])
    for n in range(5, -1, -1):
        series = series * square + SINE[n]
    return radius * (turn * series)


def lane_next(main, side, lane):
    main, side = pltpu.roll(main, LANES - 1, 1), pltpu.roll(side, LANES - 1, 1)
    last = lane == LANES - 1
    return jnp.where(last, side, main), jnp.where(last, main, side)


def lane_prev(main, side, lane):
    main, side = pltpu.roll(main, 1, 1), pltpu.roll(side, 1, 1)
    first = lane == 0
    return jnp.where(first, side, main), jnp.where(first, main, side)


def pick(index, lane_source):
    return jnp.take_along_axis(lane_source, index, axis=1, mode="promise_in_bounds")


def kernel(
    field_ref, info_ref, kappa_ref, mass_ref, seed_ref, order_ref, outn, energy_ref,
    nat, halo, turned_nat, edge_planes, pack, strip_l, strip_r, seedbuf, seedmap, noise, fld, stf, inf, inv, scl, kd, fac, delta, acc, sums,
    load_sem, send_sem, recv_sem, esend, erecv, known,
):
    r, c = lax.axis_index("row"), lax.axis_index("col")
    sub, lane = tile()

    def at(dr, dc):
        return (lax.rem(r + (dr + 8), 8), lax.rem(c + (dc + 16), 16))

    barrier = pltpu.get_barrier_semaphore()
    peers = [at(*where) for where in NEIGHBOURS]
    peers += [at(0, k) for k in range(2, 15)] + [at(k, 0) for k in range(2, 7)]
    for peer in peers[:8]:
        pl.semaphore_signal(barrier, inc=1, device_id=peer, device_id_type=MESH)

    sources = (field_ref.at[0], info_ref, kappa_ref, mass_ref)
    loads = []
    for i in range(4):
        for k in range(4):
            loads.append(
                pltpu.make_async_copy(
                    sources[i].at[:, pl.ds(LANES * k, LANES)], nat.at[i, k, pl.ds(HALO, TR)], load_sem.at[i, k]
                )
            )
            loads[-1].start()

    for peer in peers[8:]:
        pl.semaphore_signal(barrier, inc=1, device_id=peer, device_id_type=MESH)

    own = jnp.zeros((8, LANES), jnp.int32)
    for t in range(SWEEPS):
        for colour in range(COLOURS):
            seed = jnp.int32(0)
            for k in range(COLOURS):
                seed = seed + jnp.where(order_ref[k] == colour, seed_ref[t, 0, k], 0)
            own = jnp.where(sub == t * COLOURS + colour, seed, own)
    seedbuf[4] = own

    pl.semaphore_wait(barrier, len(peers))
    copies = []

    def send(source, target, where):
        n = len(copies)
        copies.append(
            pltpu.make_async_remote_copy(
                src_ref=source,
                dst_ref=target,
                send_sem=send_sem.at[n],
                recv_sem=recv_sem.at[n],
                device_id=at(*where),
                device_id_type=MESH,
            )
        )
        copies[-1].start()

    for dr, dc in NEIGHBOURS:
        send(seedbuf.at[4], seedbuf.at[(1 - dr) * 3 + 1 - dc], (dr, dc))
    for load in loads:
        load.wait()
    for g in range(TR // 8):
        rows = pl.ds(HALO + 8 * g, 8)
        total = jnp.zeros((8, LANES), jnp.float32)
        for i in range(4):
            right = pltpu.roll(nat[i, 3, rows, :], 16 * i + 16, 1)
            left = pltpu.roll(nat[i, 0, rows, :], 64 + 16 * i, 1)
            total = jnp.where((lane >= 16 * i) & (lane < 16 * i + 16), right, total)
            total = jnp.where((lane >= 64 + 16 * i) & (lane < 80 + 16 * i), left, total)
        pack[pl.ds(8 * g, 8), :] = total
    def splat(slot, n):
        return jnp.broadcast_to(seedbuf[slot, n : n + 1, :], (8, LANES))

    for n in range(8):
        seedmap[n, 0, 1] = splat(4, n)
    for dr in (-1, 0, 1):
        mine = {-1: pl.ds(0, HALO), 0: pl.ds(0, TR), 1: pl.ds(TR - HALO, HALO)}[dr]
        theirs = {-1: pl.ds(HALO + TR, HALO), 0: pl.ds(HALO, TR), 1: pl.ds(0, HALO)}[dr]
        send(pack.at[mine], strip_l.at[theirs], (dr, 1))
        send(pack.at[mine], strip_r.at[theirs], (dr, -1))
    send(nat.at[:, :, pl.ds(HALO, HALO)], halo.at[1, :, :, pl.ds(HALO, HALO)], (-1, 0))
    send(nat.at[:, :, pl.ds(TR, HALO)], halo.at[0, :, :, pl.ds(0, HALO)], (1, 0))
    for k in range(1, 8):
        pl.semaphore_signal(known, inc=1, device_id=at(k, 0), device_id_type=MESH)

    zero = jnp.zeros((8, LANES), jnp.float32)

    one = jnp.ones((8, LANES), jnp.float32)

    def clear(n, _):
        for i in range(4):
            nat[i, lax.rem(n, 4), pl.ds(pl.multiple_of(8 * (n // 4) + jnp.where(n >= 8, TR, 0), 8), 8), :] = one
        for v in range(2):
            for buffer in (fld, inv):
                buffer[n, v, 0:PAD, :] = zero
                buffer[n, v, PAD + ROWS : PADDED, :] = zero
            for i in range(PHASES):
                scl[i, n, v, 0:PAD, :] = zero
                scl[i, n, v, PAD + ROWS : PADDED, :] = zero
        return 0

    def clear_moves(i, _):
        for n in range(16):
            for v in range(2):
                kd[i, n, v, 0:PAD, :] = zero
                kd[i, n, v, PAD + ROWS : PADDED, :] = zero
                if n in (10, 11, 14, 15):
                    for g in range(GROUPS):
                        kd[i, n, v, PAD + 8 * g : PAD + 8 * g + 8, :] = zero
        return 0

    lax.fori_loop(0, PHASES - 1, clear_moves, 0)
    lax.fori_loop(0, 16, clear, 0)

    block = lane // 32
    split = [4 * (lane & 31) + ((block - k) & 3) for k in range(4)]
    edge = lane < 64
    used = (lane < 4) | (lane >= 124)

    def finish_planes(g, v):
        rows = pl.ds(8 * g, 8)
        padded = pl.ds(8 * g + PAD, 8)
        for n in range(16):
            mass = inv[n, v, padded, :]
            stf[n, v, rows, :] = stf[n, v, rows, :] * mass + 4.0
            inv[n, v, padded, :] = 1.0 / mass

    def place_of(g):
        rows, padded = pl.ds(8 * g, 8), pl.ds(8 * g + PAD, 8)
        return (fld, padded), (inf, rows), (stf, rows), (inv, padded)

    def gather_columns(g, load):
        for rho in range(4):
            for i in range(4):
                for k in range(4):
                    turned_nat[g, i, rho, k] = pick(split[k], load(i, k, rho))

    def turn_columns(g, part=None):
        for rho in range(4):
            for i, (ref, where) in enumerate(place_of(g)):
                chunks = [turned_nat[g, i, rho, k] for k in range(4)]
                for kappa in range(4):
                    m = chunks[(-kappa) & 3]
                    for b in range(1, 4):
                        m = jnp.where(block == b, chunks[(b - kappa) & 3], m)
                    m = pltpu.roll(m, LANES - 32 * kappa, 1) if kappa else m
                    if part is None:
                        ref[4 * rho + kappa, 0, where, :] = m
                    else:
                        edge_planes[i, 4 * rho + kappa, g // 4] = m

    def blend(g, part):
        rows, padded = pl.ds(8 * g, 8), pl.ds(8 * g + PAD, 8)
        for n in range(16):
            mass = edge_planes[3, n, g // 4]
            new = (edge_planes[0, n, g // 4], edge_planes[1, n, g // 4], edge_planes[2, n, g // 4] * mass + 4.0, 1.0 / mass)
            for ref, where, value in zip((fld, inf, stf, inv), (padded, rows, rows, padded), new):
                ref[n, 0, where, :] = jnp.where(part, value, ref[n, 0, where, :])

    def side_planes(g):
        for rho in range(4):
            natural = pl.ds(32 * g + rho, 8, stride=4)
            mixed = jnp.where(edge, strip_l[natural, :], strip_r[natural, :])
            for kappa in range(4):
                for i, (ref, where) in enumerate(place_of(g)):
                    index = 16 * i + 4 * (lane & 3) + kappa + jnp.where(edge, 64, 0)
                    ref[4 * rho + kappa, 1, where, :] = jnp.where(used, pick(index, mixed), 0.0 if i < 2 else 1.0)

    def draw(g, group_class, v):
        for rho in range(4):
            row = 4 * ((sub + (8 * g + 28)) & 31) + rho
            for kappa in range(4):
                colour = 2 * (rho // 2) + kappa // 2
                offset = 2 * (row * TC + 4 * lane + kappa)
                for t in range(SWEEPS):
                    seeds = seedmap[t * COLOURS + colour, v, group_class]
                    noise[t, 4 * rho + kappa, v, pl.ds(pl.multiple_of(8 * g, 8), 8), :] = gaussian(seeds + offset)

    def inner(g, _):
        draw(g, 1, 0)
        return 0

    lax.fori_loop(1, GROUPS - 1, inner, 0)

    for g in range(GROUPS):
        gather_columns(g, lambda i, k, rho, g=g: nat[i, k, pl.ds(32 * g + rho, 8, stride=4), :])
    for g in range(GROUPS):
        turn_columns(g)
    for g in range(GROUPS):
        finish_planes(g, 0)
    for copy in copies[:8]:
        copy.wait()
    for n in range(8):
        seedmap[n, 0, 0] = jnp.where(sub < 4, splat(1, n), splat(4, n))
        seedmap[n, 0, 2] = jnp.where(sub < 4, splat(4, n), splat(7, n))
        rows = [jnp.where(lane < 64, splat(3 * a + 2, n), splat(3 * a, n)) for a in range(3)]
        seedmap[n, 1, 0] = jnp.where(sub < 4, rows[0], rows[1])
        seedmap[n, 1, 1] = rows[1]
        seedmap[n, 1, 2] = jnp.where(sub < 4, rows[1], rows[2])
    draw(0, 0, 0)
    draw(GROUPS - 1, 2, 0)

    def side(g, _):
        draw(g, jnp.where(g == 0, 0, jnp.where(g == GROUPS - 1, 2, 1)), 1)
        return 0

    lax.fori_loop(0, GROUPS, side, 0)

    for copy in copies[8:14]:
        copy.wait()
    for g in range(GROUPS):
        side_planes(g)
    for g in range(GROUPS):
        finish_planes(g, 1)

    def around(ref, rho, kappa, base):
        up = (4 * ((rho + 3) % 4) + kappa, base - 1 if rho == 0 else base)
        down = (4 * ((rho + 1) % 4) + kappa, base + 1 if rho == 3 else base)
        here = pl.ds(base, 8)
        left = [ref[4 * rho + (kappa + 3) % 4, v, here, :] for v in range(2)]
        right = [ref[4 * rho + (kappa + 1) % 4, v, here, :] for v in range(2)]
        if kappa == 0:
            left = lane_prev(*left, lane)
        if kappa == 3:
            right = lane_next(*right, lane)
        return [
            ref[up[0], v, pl.ds(up[1], 8), :] + ref[down[0], v, pl.ds(down[1], 8), :] + left[v] + right[v]
            for v in range(2)
        ]

    def is_own(g):
        j = sub + 8 * g
        return (j >= 4) & (j < 36)

    def first(g, total):
        base = 8 * g + PAD
        rows = pl.ds(8 * g, 8)
        here = pl.ds(base, 8)
        part = zero
        for rho in range(4):
            for kappa in range(4):
                n = 4 * rho + kappa
                near = around(fld, rho, kappa, base)
                for v in range(2):
                    value = fld[n, v, here, :]
                    applied = stf[n, v, rows, :] * value - near[v]
                    scaled = inv[n, v, here, :] * applied
                    scl[0, n, v, here, :] = scaled
                    if v == 0:
                        part = part + (0.5 * scaled * applied - inf[n, v, rows, :] * value)
        return total + jnp.where(is_own(g), part, 0.0)


    def factors(g):
        base = 8 * g + PAD
        rows = pl.ds(8 * g, 8)
        here = pl.ds(base, 8)
        for colour in range(COLOURS):
            top, left = 2 * (colour // 2), 2 * (colour % 2)
            corner = [(top + n // 2, left + n % 2) for n in range(4)]
            near = [around(inv, rho, kappa, base) for rho, kappa in corner]
            for v in range(2):
                s = [stf[4 * rho + kappa, v, rows, :] for rho, kappa in corner]
                w = [inv[4 * rho + kappa, v, here, :] for rho, kappa in corner]
                sw = [s[n] * w[n] for n in range(4)]
                q = {(n, n): s[n] * sw[n] + near[n][v] for n in range(4)}
                for a, b in ((1, 0), (2, 0), (3, 1), (3, 2)):
                    q[a, b] = -(sw[a] + sw[b])
                q[3, 0] = w[1] + w[2]
                q[2, 1] = w[0] + w[3]
                low = {}
                for a in range(4):
                    for b in range(a + 1):
                        running = q[a, b]
                        for m in range(b):
                            running = running - low[a, m] * low[b, m]
                        low[a, b] = lax.rsqrt(running) if a == b else running * low[b, b]
                for n in range(4):
                    fac[n, colour, v, rows, :] = low[n, n]
                for (a, b), n in LOWER.items():
                    fac[n, colour, v, rows, :] = low[a, b]


    def resample(i, g, total, scatter):
        t, k = i // COLOURS, lax.rem(i, COLOURS)
        colour = order_ref[k]
        a, b = lax.shift_right_logical(colour, 1), colour & 1
        low_b = jnp.full((8, LANES), b, jnp.int32) == 0
        base = 8 * g + PAD
        rows = pl.ds(8 * g, 8)
        here = pl.ds(base, 8)
        rel_row = [2 * a, 2 * a + 1, (2 * a + 2) & 3, (2 * a + 3) & 3]
        rel_col = [2 * b, 2 * b + 1, (2 * b + 2) & 3, (2 * b + 3) & 3]
        above = pl.ds(base - jnp.where(a == 0, 1, 0), 8)
        below = pl.ds(base + jnp.where(a == 1, 1, 0), 8)

        def read(p, q, where=here):
            return [scl[i, 4 * rel_row[p] + rel_col[q], v, where, :] for v in range(2)]

        node = [[read(p, q) for q in range(2)] for p in range(2)]
        up = [read(3, q, above) for q in range(2)]
        down = [read(2, q, below) for q in range(2)]
        left, right = [], []
        for p in range(2):
            raw = read(p, 3)
            moved = lane_prev(*raw, lane)
            left.append([jnp.where(low_b, moved[v], raw[v]) for v in range(2)])
            raw = read(p, 2)
            moved = lane_next(*raw, lane)
            right.append([jnp.where(low_b, raw[v], moved[v]) for v in range(2)])
        moves = []
        for v in range(2):
            f, drawn = [], []
            inverse = [fac[n, colour, v, rows, :] for n in range(4)]
            low = {key: fac[n, colour, v, rows, :] for key, n in LOWER.items()}
            for n in range(4):
                p, q = n // 2, n % 2
                place = 4 * rel_row[p] + rel_col[q]
                near = node[1 - p][q][v] + node[p][1 - q][v]
                near = near + (down if p else up)[q][v] + (right if q else left)[p][v]
                running = inf[place, v, rows, :] - stf[place, v, rows, :] * node[p][q][v] + near
                for m in range(n):
                    running = running - low[n, m] * f[m]
                f.append(running * inverse[n])
                drawn.append(noise[t, place, v, rows, :])
            target = [f[n] + drawn[n] for n in range(4)]
            if v == 0 and scatter:
                part = (drawn[0] - f[0]) * target[0]
                for n in range(1, 4):
                    part = part + (drawn[n] - f[n]) * target[n]
                total = total + jnp.where(is_own(g), 0.5 * part, 0.0)
            move = [None] * 4
            for n in reversed(range(4)):
                running = target[n]
                for m in range(n + 1, 4):
                    running = running - low[m, n] * move[m]
                move[n] = running * inverse[n]
                if v == 0:
                    delta[i, n, rows, :] = move[n]
            if scatter:
                for n in range(4):
                    p, q = n // 2, n % 2
                    place = 4 * rel_row[p] + rel_col[q]
                    kd[i, 4 * p + q, v, here, :] = move[n ^ 1] + move[n ^ 2] - stf[place, v, rows, :] * move[n]
                for q in range(2):
                    kd[i, 12 + q, v, here, :] = move[q]
                    kd[i, 8 + q, v, here, :] = move[2 + q]
            moves.append(move)
        if scatter:
            for p in range(2):
                raw = [moves[v][2 * p] for v in range(2)]
                moved = lane_next(*raw, lane)
                for v in range(2):
                    kd[i, 4 * p + 3, v, here, :] = jnp.where(low_b, moved[v], raw[v])
                raw = [moves[v][2 * p + 1] for v in range(2)]
                moved = lane_prev(*raw, lane)
                for v in range(2):
                    kd[i, 4 * p + 2, v, here, :] = jnp.where(low_b, raw[v], moved[v])
        return total

    def spread(i, g):
        colour = order_ref[lax.rem(i, COLOURS)]
        a, b = lax.shift_right_logical(colour, 1), colour & 1
        base = 8 * g + PAD
        here = pl.ds(base, 8)
        for rho in range(4):
            where = here
            if rho == 3:
                where = pl.ds(base + jnp.where(a == 0, 1, 0), 8)
            if rho == 0:
                where = pl.ds(base - jnp.where(a == 1, 1, 0), 8)
            for kappa in range(4):
                n = 4 * rho + kappa
                place = 4 * ((rho + 4 - 2 * a) & 3) + ((kappa + 4 - 2 * b) & 3)
                for v in range(2):
                    scl[i + 1, n, v, here, :] = scl[i, n, v, here, :] - inv[n, v, here, :] * kd[i, place, v, where, :]

    inside, rim, every = range(1, GROUPS - 1), (0, GROUPS - 1), range(GROUPS)

    def phase(i, groups, counted):
        total = zero
        for g in groups:
            change = resample(i, g, zero, True)
            total = total + change if g in counted else total
        acc[i + 1] = total if counted is inside else acc[i + 1] + total
        for g in groups:
            spread(i, g)
        return 0

    total = zero
    for g in every:
        part = first(g, zero)
        total = total + part if g in inside else total
    acc[0] = total
    for g in every:
        factors(g)
    lax.fori_loop(0, PHASES - 1, lambda i, _: phase(i, every, inside), 0)

    for copy in copies[14:]:
        copy.wait()
    for g, side in ((0, 0), (GROUPS - 1, 1)):
        gather_columns(g, lambda i, k, rho, side=side: halo[side, i, k, pl.ds(rho, 8, stride=4), :])
    for g in rim:
        turn_columns(g, True)
    blend(0, sub < 4)
    blend(GROUPS - 1, sub >= 4)
    for g in rim:
        acc[0] = first(g, acc[0])
    for g in rim:
        factors(g)
    lax.fori_loop(0, PHASES - 1, lambda i, _: phase(i, rim, rim), 0)

    line = jnp.zeros((1, LANES), jnp.float32)
    for k in range(PHASES):
        change = jnp.sum(jnp.sum(acc[k], axis=0, keepdims=True), axis=1, keepdims=True)
        line = line + jnp.where(lane[0:1] >= k, change, 0.0)
    me = 16 * r + c
    mine = sums.at[pl.ds(me, 1)]
    sums[pl.ds(me, 1), :] = line
    pl.semaphore_wait(known, 7)

    def share(k, _):
        row, col = lax.rem(k, 32) // 4, 8 * lax.rem(k // 2, 2) + 2 * (k // 32) + lax.rem(k, 2)

        @pl.when(16 * row + col != me)
        def _():
            pltpu.make_async_remote_copy(
                src_ref=mine, dst_ref=mine, send_sem=esend, recv_sem=erecv, device_id=(row, col), device_id_type=MESH
            ).start()

        return 0

    lax.fori_loop(0, DEVICES, share, 0)

    for g in every:
        resample(PHASES - 1, g, zero, False)

    turn_of = []
    for colour in range(COLOURS):
        turn = jnp.int32(0)
        for k in range(COLOURS):
            turn = jnp.where(order_ref[k] == colour, jnp.int32(k), turn)
        turn_of.append(turn)
    merge = [32 * (((lane & 3) + k) & 3) + lane // 4 for k in range(4)]

    def natural_rows(h, _):
        for rho in range(4):
            shifted = []
            for kappa in range(4):
                turn = turn_of[2 * (rho // 2) + kappa // 2]
                n = 2 * (rho % 2) + kappa % 2
                value = fld[4 * rho + kappa, 0, pl.ds(8 * h + PAD + 4, 8), :]
                value = value + delta[turn, n, pl.ds(8 * h + 4, 8), :]
                value = value + delta[turn + COLOURS, n, pl.ds(8 * h + 4, 8), :]
                shifted.append(pltpu.roll(value, 32 * kappa, 1) if kappa else value)
            for k in range(4):
                m = shifted[(-k) & 3]
                for b in range(1, 4):
                    m = jnp.where(block == b, shifted[(b - k) & 3], m)
                outn[k, pl.ds(32 * h + rho, 8, stride=4), :] = pick(merge[k], m)
        return 0

    lax.fori_loop(0, 4, natural_rows, 0)
    others = sums.at[pl.ds(0, DEVICES - 1)]
    pltpu.make_async_remote_copy(
        src_ref=others, dst_ref=others, send_sem=esend, recv_sem=erecv, device_id=at(0, 1), device_id_type=MESH
    ).wait()
    energy_ref[...] = jnp.broadcast_to(jnp.sum(sums[...], axis=0, keepdims=True) * (1.0 / NODES), (8, LANES))


def deliver(field_ref, energy_ref, out_ref, out_energy_ref, store_sem):
    stores = [
        pltpu.make_async_copy(field_ref.at[k], out_ref.at[0, :, pl.ds(LANES * k, LANES)], store_sem.at[k])
        for k in range(4)
    ]
    for store in stores:
        store.start()
    line = energy_ref[0:1, :]
    out_energy_ref[0] = line[:, 0:COLOURS]
    out_energy_ref[1] = pltpu.roll(line, LANES - COLOURS, 1)[:, 0:COLOURS]
    for store in stores:
        store.wait()


def local(initial_field, information, kappa_squared, lumped_mass, noise_seeds, colour_order):
    f32, i32 = jnp.float32, jnp.int32
    anywhere = pl.BlockSpec(memory_space=pltpu.HBM)
    scalar = pl.BlockSpec(memory_space=pltpu.SMEM)
    dma = pltpu.SemaphoreType.DMA
    seeds = noise_seeds.reshape(SWEEPS, COLOURS, 1).transpose(0, 2, 1)
    vmem = pl.BlockSpec(memory_space=pltpu.VMEM)
    arrays = (initial_field, information, kappa_squared, lumped_mass)
    chunks, line = pl.pallas_call(
        kernel,
        out_shape=(jax.ShapeDtypeStruct((4, TR, LANES), f32), jax.ShapeDtypeStruct((8, LANES), f32)),
        in_specs=[anywhere] * 4 + [scalar] * 2,
        out_specs=(vmem, vmem),
        scratch_shapes=[
            pltpu.VMEM((4, 4, EXT, LANES), f32),
            pltpu.VMEM((2, 4, 4, 2 * HALO, LANES), f32),
            pltpu.VMEM((GROUPS, 4, 4, 4, 8, LANES), f32),
            pltpu.VMEM((4, 16, 2, 8, LANES), f32),
            pltpu.VMEM((TR, LANES), f32),
            pltpu.VMEM((EXT, LANES), f32),
            pltpu.VMEM((EXT, LANES), f32),
            pltpu.VMEM((9, 8, LANES), i32),
            pltpu.VMEM((8, 2, 3, 8, LANES), i32),
            pltpu.VMEM((SWEEPS, 16, 2, ROWS, LANES), f32),
            pltpu.VMEM((16, 2, PADDED, LANES), f32),
            pltpu.VMEM((16, 2, ROWS, LANES), f32),
            pltpu.VMEM((16, 2, ROWS, LANES), f32),
            pltpu.VMEM((16, 2, PADDED, LANES), f32),
            pltpu.VMEM((PHASES, 16, 2, PADDED, LANES), f32),
            pltpu.VMEM((PHASES - 1, 16, 2, PADDED, LANES), f32),
            pltpu.VMEM((10, COLOURS, 2, ROWS, LANES), f32),
            pltpu.VMEM((PHASES, 4, ROWS, LANES), f32),
            pltpu.VMEM((PHASES, 8, LANES), f32),
            pltpu.VMEM((DEVICES, LANES), f32),
            dma((4, 4)),
            dma((16,)),
            dma((16,)),
            dma,
            dma,
            pltpu.SemaphoreType.REGULAR,
        ],
        compiler_params=pltpu.CompilerParams(collective_id=0, has_side_effects=True, vmem_limit_bytes=VMEM_LIMIT),
        name="gibbs",
    )(*(pltpu.with_memory_space_constraint(a, pltpu.HBM) for a in (*arrays, seeds, colour_order)))
    final_field, energies = pl.pallas_call(
        deliver,
        out_shape=(jax.ShapeDtypeStruct((1, TR, TC), f32), jax.ShapeDtypeStruct((SWEEPS, 1, COLOURS), f32)),
        in_specs=[vmem, vmem],
        out_specs=(anywhere, vmem),
        scratch_shapes=[dma((4,))],
        compiler_params=pltpu.CompilerParams(vmem_limit_bytes=VMEM_LIMIT),
        name="deliver",
    )(chunks, line)
    return final_field, energies.transpose(0, 2, 1)


def solution(mesh):
    placed = (
        P(None, "row", "col"),
        P("row", "col"),
        P("row", "col"),
        P("row", "col"),
        P("row", "col", None, None, None),
        P(),
    )
    return jax.shard_map(
        local, mesh=mesh, in_specs=placed, out_specs=(P(None, "row", "col"), P()), check_vma=False
    )
```
